16 devices in a mesh: dp: 2 (over z), cp: 8 (over y, x, core).
Axes of the slice: x: 2, y: 2, z: 2, core: 2. Of those that a mesh axis runs over, the one named last changes fastest.
Arguments:
- images: bfloat16 [64, 576, 1024], P('dp', 'cp'), parts along dimension 0
- ln1_scale: float32 [1024], replicated
- ln1_bias: float32 [1024], replicated
- w_qkv: bfloat16 [1024, 3, 16, 64], replicated
- b_qkv: float32 [3, 16, 64], replicated
- w_out: bfloat16 [16, 64, 1024], replicated
- b_out: float32 [1024], replicated
- ln2_scale: float32 [1024], replicated
- ln2_bias: float32 [1024], replicated
- w_up: bfloat16 [1024, 4096], replicated
- b_up: float32 [4096], replicated
- w_down: bfloat16 [4096, 1024], replicated
- b_down: float32 [1024], replicated
- lnf_scale: float32 [1024], replicated
- lnf_bias: float32 [1024], replicated
- pool_probe: bfloat16 [1, 1024], replicated
- pool_wq: bfloat16 [1024, 16, 64], replicated
- pool_bq: float32 [16, 64], replicated
- pool_wkv: bfloat16 [1024, 2, 16, 64], replicated
- pool_bkv: float32 [2, 16, 64], replicated
- pool_wout: bfloat16 [16, 64, 1024], replicated
- pool_bout: float32 [1024], replicated
- pool_ln_scale: float32 [1024], replicated
- pool_ln_bias: float32 [1024], replicated
- pool_w_up: bfloat16 [1024, 4096], replicated
- pool_b_up: float32 [4096], replicated
- pool_w_down: bfloat16 [4096, 1024], replicated
- pool_b_down: float32 [1024], replicated
Outputs:
- output: float32 [64, 1024], P('dp'), parts along dimension 0
There are 2 independent parts. The reference program is written for one: setup_inputs(seed, part) draws one part's arguments, and reference() takes and returns one part's arrays. A program takes and returns all parts, laid end to end along the dimension named above; an argument that names none is the same for every part.
All inputs are finite; a program needn't handle non-finite values.
Results may differ from the reference program's by a relative error of at most 0.00933342.
Values are sent between devices in bfloat16 or wider.
A program may use at most 1 GiB of HBM per device.

```python
import math
import jax
import jax.numpy as jnp
from jax import lax

IMAGES = 32
TOKENS = 576
MODEL_DIM = 1024
NUM_HEADS = 16
HEAD_DIM = 64
MLP_DIM = 4096

ROW_BLOCK = TOKENS // 16
GRID_SIDE = math.isqrt(TOKENS)


def weight_draw(rand_key, arr_shape, fan_in):
    return (jax.random.normal(rand_key, arr_shape, jnp.float32) * fan_in ** -0.5).astype(jnp.bfloat16)


def gain_draw(rand_key, arr_shape):
    return 1.0 + 0.2 * jax.random.normal(rand_key, arr_shape, jnp.float32)


def shift_draw(rand_key, arr_shape):
    return 0.2 * jax.random.normal(rand_key, arr_shape, jnp.float32)


def setup_inputs(seed: int = 0, part: int = 0) -> dict:
    root_key = jax.random.key(seed)
    halves = jax.random.split(root_key, 2)
    image_keys = jax.random.split(jax.random.fold_in(halves[0], part), 5)
    weight_keys = jax.random.split(halves[1], 27)
    wave_count = 8
    positions = jnp.arange(TOKENS)
    grid_rows = (positions // GRID_SIDE).astype(jnp.float32) / GRID_SIDE
    grid_cols = (positions % GRID_SIDE).astype(jnp.float32) / GRID_SIDE
    freq_rows = jax.random.randint(image_keys[0], (IMAGES, wave_count), 1, 4).astype(jnp.float32)
    freq_cols = jax.random.randint(image_keys[1], (IMAGES, wave_count), 0, 4).astype(jnp.float32)
    phases = jax.random.uniform(image_keys[2], (IMAGES, wave_count), jnp.float32, 0.0, 2.0 * math.pi)
    wave_rows = jnp.cos(2.0 * math.pi * (freq_rows[:, :, None] * grid_rows + freq_cols[:, :, None] * grid_cols) + phases[:, :, None])
    directions = jax.random.normal(image_keys[3], (IMAGES, wave_count, MODEL_DIM), jnp.float32) * (2.0 / wave_count) ** 0.5
    wave_field = jnp.einsum("bwn,bwd->bnd", wave_rows, directions)
    noise_part = jax.random.normal(image_keys[4], (IMAGES, TOKENS, MODEL_DIM), jnp.float32)
    return {
        "images": (wave_field + 0.5 * noise_part).astype(jnp.bfloat16),
        "ln1_scale": gain_draw(weight_keys[0], (MODEL_DIM,)),
        "ln1_bias": shift_draw(weight_keys[1], (MODEL_DIM,)),
        "w_qkv": weight_draw(weight_keys[2], (MODEL_DIM, 3, NUM_HEADS, HEAD_DIM), MODEL_DIM),
        "b_qkv": shift_draw(weight_keys[3], (3, NUM_HEADS, HEAD_DIM)),
        "w_out": weight_draw(weight_keys[4], (NUM_HEADS, HEAD_DIM, MODEL_DIM), MODEL_DIM),
        "b_out": shift_draw(weight_keys[5], (MODEL_DIM,)),
        "ln2_scale": gain_draw(weight_keys[6], (MODEL_DIM,)),
        "ln2_bias": shift_draw(weight_keys[7], (MODEL_DIM,)),
        "w_up": weight_draw(weight_keys[8], (MODEL_DIM, MLP_DIM), MODEL_DIM),
        "b_up": shift_draw(weight_keys[9], (MLP_DIM,)),
        "w_down": weight_draw(weight_keys[10], (MLP_DIM, MODEL_DIM), MLP_DIM),
        "b_down": shift_draw(weight_keys[11], (MODEL_DIM,)),
        "lnf_scale": gain_draw(weight_keys[12], (MODEL_DIM,)),
        "lnf_bias": shift_draw(weight_keys[13], (MODEL_DIM,)),
        "pool_probe": jax.random.normal(weight_keys[14], (1, MODEL_DIM), jnp.float32).astype(jnp.bfloat16),
        "pool_wq": weight_draw(weight_keys[15], (MODEL_DIM, NUM_HEADS, HEAD_DIM), MODEL_DIM),
        "pool_bq": shift_draw(weight_keys[16], (NUM_HEADS, HEAD_DIM)),
        "pool_wkv": weight_draw(weight_keys[17], (MODEL_DIM, 2, NUM_HEADS, HEAD_DIM), MODEL_DIM),
        "pool_bkv": shift_draw(weight_keys[18], (2, NUM_HEADS, HEAD_DIM)),
        "pool_wout": weight_draw(weight_keys[19], (NUM_HEADS, HEAD_DIM, MODEL_DIM), MODEL_DIM),
        "pool_bout": shift_draw(weight_keys[20], (MODEL_DIM,)),
        "pool_ln_scale": gain_draw(weight_keys[21], (MODEL_DIM,)),
        "pool_ln_bias": shift_draw(weight_keys[22], (MODEL_DIM,)),
        "pool_w_up": weight_draw(weight_keys[23], (MODEL_DIM, MLP_DIM), MODEL_DIM),
        "pool_b_up": shift_draw(weight_keys[24], (MLP_DIM,)),
        "pool_w_down": weight_draw(weight_keys[25], (MLP_DIM, MODEL_DIM), MLP_DIM),
        "pool_b_down": shift_draw(weight_keys[26], (MODEL_DIM,)),
    }


def layer_norm(values, ln_gain, ln_shift):
    row_mean = jnp.mean(values, axis=-1, keepdims=True)
    centered = values - row_mean
    variance = jnp.mean(centered * centered, axis=-1, keepdims=True)
    return centered * lax.rsqrt(variance + 1e-6) * ln_gain + ln_shift


def reference(images, ln1_scale, ln1_bias, w_qkv, b_qkv, w_out, b_out, ln2_scale, ln2_bias, w_up, b_up, w_down, b_down, lnf_scale, lnf_bias, pool_probe, pool_wq, pool_bq, pool_wkv, pool_bkv, pool_wout, pool_bout, pool_ln_scale, pool_ln_bias, pool_w_up, pool_b_up, pool_w_down, pool_b_down):
    score_scale = HEAD_DIM ** -0.5
    probe_q = (jnp.einsum("od,dhe->he", pool_probe.astype(jnp.float32), pool_wq.astype(jnp.float32)) + pool_bq).astype(jnp.bfloat16)

    def one_image(image_tokens):
        resid_in = image_tokens.astype(jnp.float32)
        normed = layer_norm(resid_in, ln1_scale, ln1_bias).astype(jnp.bfloat16)
        qkv = (jnp.einsum("nd,dshe->snhe", normed.astype(jnp.float32), w_qkv.astype(jnp.float32)) + b_qkv[:, None]).astype(jnp.bfloat16)
        key_rows = qkv[1].astype(jnp.float32)
        value_rows = qkv[2].astype(jnp.float32)

        def attend_rows(query_rows):
            scores = jnp.einsum("qhe,khe->hqk", query_rows.astype(jnp.float32), key_rows) * score_scale
            weights = jnp.exp(scores - jnp.max(scores, axis=-1, keepdims=True))
            value_sum = jnp.einsum("hqk,khe->hqe", weights.astype(jnp.bfloat16).astype(jnp.float32), value_rows)
            return value_sum / jnp.sum(weights, axis=-1)[:, :, None]

        blocks = lax.map(attend_rows, qkv[0].reshape(TOKENS // ROW_BLOCK, ROW_BLOCK, NUM_HEADS, HEAD_DIM))
        context = blocks.transpose(1, 0, 2, 3).reshape(NUM_HEADS, TOKENS, HEAD_DIM).astype(jnp.bfloat16)
        attn_out = jnp.einsum("hne,hed->nd", context.astype(jnp.float32), w_out.astype(jnp.float32)) + b_out
        resid_mid = (resid_in + attn_out).astype(jnp.bfloat16)
        normed_mid = layer_norm(resid_mid.astype(jnp.float32), ln2_scale, ln2_bias).astype(jnp.bfloat16)
        hidden = jax.nn.gelu(jnp.dot(normed_mid, w_up, preferred_element_type=jnp.float32) + b_up, approximate=True).astype(jnp.bfloat16)
        layer_out = (resid_mid.astype(jnp.float32) + jnp.dot(hidden, w_down, preferred_element_type=jnp.float32) + b_down).astype(jnp.bfloat16)
        tokens_out = layer_norm(layer_out.astype(jnp.float32), lnf_scale, lnf_bias).astype(jnp.bfloat16)
        pool_kv = (jnp.einsum("nd,dshe->snhe", tokens_out.astype(jnp.float32), pool_wkv.astype(jnp.float32)) + pool_bkv[:, None]).astype(jnp.bfloat16)
        pool_scores = jnp.einsum("he,nhe->hn", probe_q.astype(jnp.float32), pool_kv[0].astype(jnp.float32)) * score_scale
        pool_weights = jnp.exp(pool_scores - jnp.max(pool_scores, axis=-1, keepdims=True))
        pool_sum = jnp.einsum("hn,nhe->he", pool_weights.astype(jnp.bfloat16).astype(jnp.float32), pool_kv[1].astype(jnp.float32))
        pooled = (pool_sum / jnp.sum(pool_weights, axis=-1)[:, None]).astype(jnp.bfloat16)
        pooled_out = (jnp.einsum("he,hed->d", pooled.astype(jnp.float32), pool_wout.astype(jnp.float32)) + pool_bout).astype(jnp.bfloat16)
        normed_out = layer_norm(pooled_out.astype(jnp.float32), pool_ln_scale, pool_ln_bias).astype(jnp.bfloat16)
        hidden_out = jax.nn.gelu(jnp.dot(normed_out[None], pool_w_up, preferred_element_type=jnp.float32)[0] + pool_b_up, approximate=True).astype(jnp.bfloat16)
        return pooled_out.astype(jnp.float32) + jnp.dot(hidden_out[None], pool_w_down, preferred_element_type=jnp.float32)[0] + pool_b_down

    return lax.map(one_image, images)
```

```python
import jax
import jax.numpy as jnp
from jax import lax
from jax.sharding import PartitionSpec as P

EPSILON = 1e-6


def layer_norm(values, ln_gain, ln_shift):
    row_mean = jnp.mean(values, axis=-1, keepdims=True)
    centered = values - row_mean
    variance = jnp.mean(centered * centered, axis=-1, keepdims=True)
    return centered * lax.rsqrt(variance + EPSILON) * ln_gain + ln_shift


def project(normed, weight, bias_vec):
    return (jnp.einsum("bnd,dhe->bnhe", normed, weight, preferred_element_type=jnp.float32) + bias_vec).astype(jnp.bfloat16)


def attend(queries, key_rows, value_rows, score_scale):
    scores = jnp.einsum("bqhe,bkhe->bhqk", queries, key_rows, preferred_element_type=jnp.float32) * score_scale
    weights = jnp.exp(scores - jnp.max(scores, axis=-1, keepdims=True))
    value_sum = jnp.einsum("bhqk,bkhe->bhqe", weights.astype(jnp.bfloat16), value_rows, preferred_element_type=jnp.float32)
    return (value_sum / jnp.sum(weights, axis=-1)[..., None]).astype(jnp.bfloat16)


def token_tail(resid_in, context, w_out, b_out, ln2_scale, ln2_bias, w_up, b_up, w_down, b_down, lnf_scale, lnf_bias):
    attn_out = jnp.einsum("cirf,ife->cre", context, w_out, preferred_element_type=jnp.float32) + b_out
    resid_mid = (resid_in + attn_out).astype(jnp.bfloat16)
    normed_mid = layer_norm(resid_mid.astype(jnp.float32), ln2_scale, ln2_bias).astype(jnp.bfloat16)
    hidden = jax.nn.gelu(jnp.einsum("bnd,df->bnf", normed_mid, w_up, preferred_element_type=jnp.float32) + b_up, approximate=True).astype(jnp.bfloat16)
    layer_out = (resid_mid.astype(jnp.float32) + jnp.einsum("bnf,fd->bnd", hidden, w_down, preferred_element_type=jnp.float32) + b_down).astype(jnp.bfloat16)
    return layer_norm(layer_out.astype(jnp.float32), lnf_scale, lnf_bias).astype(jnp.bfloat16)


def pool_stats(tokens_out, pool_probe, pool_wq, pool_bq, pool_wkv, pool_bkv, score_scale):
    probe_q = (jnp.einsum("od,dhe->he", pool_probe, pool_wq, preferred_element_type=jnp.float32) + pool_bq).astype(jnp.bfloat16)
    pool_keys = project(tokens_out, pool_wkv[:, 0], pool_bkv[0])
    pool_vals = project(tokens_out, pool_wkv[:, 1], pool_bkv[1])
    pool_scores = jnp.einsum("he,bnhe->bhn", probe_q, pool_keys, preferred_element_type=jnp.float32) * score_scale
    local_max = jnp.max(pool_scores, axis=-1)
    pool_weights = jnp.exp(pool_scores - local_max[..., None])
    local_val = jnp.einsum("bhn,bnhe->bhe", pool_weights.astype(jnp.bfloat16), pool_vals, preferred_element_type=jnp.float32)
    return jnp.concatenate([local_max[..., None], jnp.sum(pool_weights, axis=-1)[..., None], local_val], axis=-1)


def pool_finish(gathered, pool_wout, pool_bout, pool_ln_scale, pool_ln_bias, pool_w_up, pool_b_up, pool_w_down, pool_b_down):
    group_max = jnp.max(gathered[..., 0], axis=0)
    factors = jnp.exp(gathered[..., 0] - group_max)
    total_sum = jnp.sum(factors * gathered[..., 1], axis=0)
    total_val = jnp.sum(factors[..., None] * gathered[..., 2:], axis=0)
    pooled = (total_val / total_sum[..., None]).astype(jnp.bfloat16)
    pooled_out = (jnp.einsum("bhe,hed->bd", pooled, pool_wout, preferred_element_type=jnp.float32) + pool_bout).astype(jnp.bfloat16)
    normed_out = layer_norm(pooled_out.astype(jnp.float32), pool_ln_scale, pool_ln_bias).astype(jnp.bfloat16)
    hidden_out = jax.nn.gelu(jnp.dot(normed_out, pool_w_up, preferred_element_type=jnp.float32) + pool_b_up, approximate=True).astype(jnp.bfloat16)
    return pooled_out.astype(jnp.float32) + jnp.dot(hidden_out, pool_w_down, preferred_element_type=jnp.float32) + pool_b_down


def solution(mesh):
    group_size = mesh.shape["cp"]

    def device_step(images, ln1_scale, ln1_bias, w_qkv, b_qkv, w_out, b_out, ln2_scale, ln2_bias, w_up, b_up, w_down, b_down, lnf_scale, lnf_bias, pool_probe, pool_wq, pool_bq, pool_wkv, pool_bkv, pool_wout, pool_bout, pool_ln_scale, pool_ln_bias, pool_w_up, pool_b_up, pool_w_down, pool_b_down):
        score_scale = w_qkv.shape[-1] ** -0.5
        n_img, n_tok, width = images.shape
        own = n_img // group_size
        pieces = lax.all_to_all(images.reshape(group_size, own, n_tok, width), "cp", split_axis=0, concat_axis=0)
        images = pieces.transpose(1, 0, 2, 3).reshape(own, group_size * n_tok, width)
        resid_in = images.astype(jnp.float32)
        normed = layer_norm(resid_in, ln1_scale, ln1_bias).astype(jnp.bfloat16)
        queries = project(normed, w_qkv[:, 0], b_qkv[0])
        key_rows = project(normed, w_qkv[:, 1], b_qkv[1])
        value_rows = project(normed, w_qkv[:, 2], b_qkv[2])
        context = attend(queries, key_rows, value_rows, score_scale)
        tokens_out = token_tail(resid_in, context, w_out, b_out, ln2_scale, ln2_bias, w_up, b_up, w_down, b_down, lnf_scale, lnf_bias)
        local_stats = pool_stats(tokens_out, pool_probe, pool_wq, pool_bq, pool_wkv, pool_bkv, score_scale)
        embedding = pool_finish(local_stats[None], pool_wout, pool_bout, pool_ln_scale, pool_ln_bias, pool_w_up, pool_b_up, pool_w_down, pool_b_down)
        return lax.all_gather(embedding, "cp", tiled=True)

    in_specs = (P("dp", "cp", None),) + (P(),) * 27
    return jax.shard_map(device_step, mesh=mesh, in_specs=in_specs, out_specs=P("dp", None), check_vma=False)
```

```python
import functools

import jax
import jax.numpy as jnp
from jax import lax
from jax.experimental import pallas as pl
from jax.experimental.pallas import tpu as pltpu
from jax.sharding import PartitionSpec as P

EPSILON = 1e-6
MESH = pl.DeviceIdType.MESH
BF16 = jnp.bfloat16
F32 = jnp.float32
LOG2E = 1.4426950408889634
CONTRACT_LAST = (((1,), (1,)), ((), ()))
CONTRACT_FIRST = (((0,), (0,)), ((), ()))

V_LN1S, V_LN1B, V_BQKV, V_BOUT, V_LN2S, V_LN2B, V_BUP, V_BDOWN = 0, 1, 2, 5, 6, 7, 8, 12
V_LNFS, V_LNFB, V_PBQ, V_PBKV, V_PBOUT, V_PLNS, V_PLNB, V_PBUP, V_PBDOWN = 13, 14, 15, 16, 18, 19, 20, 21, 25
V_ROWS = 26


def layer_norm(values, ln_gain, ln_shift):
    row_mean = jnp.mean(values, axis=-1, keepdims=True)
    centered = values - row_mean
    variance = jnp.mean(centered * centered, axis=-1, keepdims=True)
    return centered * lax.rsqrt(variance + EPSILON) * ln_gain + ln_shift


def gelu(x):
    c0 = 0.7978845608028654
    return (0.5 * x) * (1.0 + jnp.tanh(x * (c0 + (c0 * 0.044715) * (x * x))))


def dot_t(lhs, rhs):
    return lax.dot_general(lhs, rhs, CONTRACT_LAST, preferred_element_type=F32)


def dot(lhs, rhs):
    return jnp.dot(lhs, rhs, preferred_element_type=F32)


def kernel(group, own, run, images, vec, probe, wqkv_hbm, wout_hbm, wup_hbm, wdown_hbm, pwq_hbm, pwkv_hbm, pwout_hbm, pwup_hbm, pwdown_hbm,
           out_ref, xbuf, wqkv, wout, wup, wdown, pwq, pwkv, hbuf, qkv, ctx, rbuf, mbuf, acc, ublk, abuf, emb, gath,
           send_sem, recv_sem, w_sem, gsend_sem, grecv_sem):
    me = lax.axis_index("cp")
    width = 1024
    rows = group * run
    pair = 2 * run
    n_pair = group // 2

    def vrow(k):
        return vec[pl.ds(k, 1), :]

    def peer(step):
        return lax.rem(me + step, group)

    weights = ((wqkv_hbm, wqkv), (pwq_hbm, pwq), (wout_hbm, wout), (wup_hbm, wup), (wdown_hbm, wdown), (pwkv_hbm, pwkv),
               (pwout_hbm, wout), (pwup_hbm, wup), (pwdown_hbm, wdown))

    def load(k):
        return pltpu.make_async_copy(weights[k][0], weights[k][1], w_sem.at[k])

    def piece(img, step):
        dst = peer(step)
        return pltpu.make_async_remote_copy(
            src_ref=images.at[dst * own + img], dst_ref=xbuf.at[img, me],
            send_sem=send_sem.at[img, step], recv_sem=recv_sem.at[img, me],
            device_id={"cp": dst}, device_id_type=MESH)

    def local_piece(img):
        return pltpu.make_async_copy(images.at[me * own + img], xbuf.at[img, me], recv_sem.at[img, me])

    load(0).start()
    load(1).start()
    barrier = pltpu.get_barrier_semaphore()
    for step in range(1, group):
        pl.semaphore_signal(barrier, inc=1, device_id={"cp": peer(step)}, device_id_type=MESH)
    pl.semaphore_wait(barrier, group - 1)

    def send_image(img, carry):
        local_piece(img).start()
        for step in (6, 2, 4, 7, 3, 5, 1):
            piece(img, step).start()
        return carry

    lax.fori_loop(0, own, send_image, 0)
    for k in range(2, 6):
        load(k).start()

    load(1).wait()
    probe_rows = jnp.broadcast_to(probe[...], (16, width))
    u = (dot_t(probe_rows, pwq[...]) + vrow(V_PBQ)).astype(BF16).astype(F32)
    head_of_lane = lax.broadcasted_iota(jnp.int32, (16, width), 1) // 64
    head_of_row = lax.broadcasted_iota(jnp.int32, (16, width), 0)
    own_head = head_of_lane == head_of_row
    ublk[...] = jnp.concatenate([jnp.where(own_head, u, 0.0), jnp.zeros((112, width), F32)], axis=0).astype(BF16)
    abuf[...] = jnp.zeros_like(abuf)

    def x_pair(img, pp):
        return jnp.concatenate([xbuf[img, 2 * pp].astype(F32), xbuf[img, 2 * pp + 1].astype(F32)], axis=0)

    def one_image(img, carry):
        first = img == 0
        last = img == own - 1

        for src in range(group):
            pltpu.make_async_copy(images.at[0], xbuf.at[img, src], recv_sem.at[img, src]).wait()
        for pp in range(n_pair):
            hbuf[pl.ds(pp * pair, pair), :] = layer_norm(x_pair(img, pp), vrow(V_LN1S), vrow(V_LN1B)).astype(BF16)

        @pl.when(first)
        def _():
            load(0).wait()

        def project(c, carry):
            qkv[c] = (dot_t(hbuf[...], wqkv[c]) + vec[pl.ds(V_BQKV + c, 1), :]).astype(BF16)
            return carry

        lax.fori_loop(0, 3, project, 0)

        lane = lax.broadcasted_iota(jnp.int32, (1, 128), 1)
        low = (lane < 64).astype(F32)
        low_b = low.astype(BF16)
        high_b = (1.0 - low).astype(BF16)
        score_mul = LOG2E * 0.125

        def head_pair(hp, carry):
            cols = pl.ds(pl.multiple_of(hp * 128, 128), 128)
            q2, k2, v2 = qkv[0, :, cols], qkv[1, :, cols], qkv[2, :, cols]

            def soft(q_half):
                scores = dot_t(q_half, k2)
                top = jnp.max(scores, axis=-1, keepdims=True)
                weight = jnp.exp2((scores - top) * score_mul)
                return weight.astype(BF16), jnp.sum(weight, axis=-1, keepdims=True)

            w_lo, l_lo = soft(q2 * low_b)
            w_hi, l_hi = soft(q2 * high_b)
            total = dot(w_lo, v2 * low_b) + dot(w_hi, v2 * high_b)
            denom = jnp.where(lane < 64, l_lo, l_hi)
            ctx[:, cols] = (total / denom).astype(BF16)
            return carry

        lax.fori_loop(0, 8, head_pair, 0)

        @pl.when(first)
        def _():
            load(2).wait()

        @pl.when(last & (own > 1))
        def _():
            pass

        acc[...] = dot(ctx[...], wout[...])

        @pl.when(last)
        def _():
            load(6).start()

        for pp in range(n_pair):
            block = pl.ds(pp * pair, pair)
            r = (x_pair(img, pp) + (acc[block, :] + vrow(V_BOUT))).astype(BF16)
            rbuf[block, :] = r
            hbuf[block, :] = layer_norm(r.astype(F32), vrow(V_LN2S), vrow(V_LN2B)).astype(BF16)

        @pl.when(first)
        def _():
            load(3).wait()
            load(4).wait()

        acc[...] = rbuf[...].astype(F32) + vrow(V_BDOWN)

        def hidden_chunk(c, carry):
            up = dot(hbuf[...], wup[:, pl.ds(pl.multiple_of(c * 1024, 1024), 1024)]) + vec[pl.ds(V_BUP + c, 1), :]
            mbuf[...] = gelu(up).astype(BF16)
            acc[...] += dot(mbuf[...], wdown[c])
            return carry

        lax.fori_loop(0, 4, hidden_chunk, 0)

        @pl.when(last)
        def _():
            load(7).start()
            load(8).start()

        for pp in range(n_pair):
            block = pl.ds(pp * pair, pair)
            y = acc[block, :].astype(BF16).astype(F32)
            hbuf[block, :] = layer_norm(y, vrow(V_LNFS), vrow(V_LNFB)).astype(BF16)

        @pl.when(first)
        def _():
            load(5).wait()

        def pool_project(c, carry):
            qkv[c] = (dot_t(hbuf[...], pwkv[c]) + vec[pl.ds(V_PBKV + c, 1), :]).astype(BF16)
            return carry

        lax.fori_loop(0, 2, pool_project, 0)
        scores = dot_t(qkv[0], ublk[...])
        top = jnp.max(scores, axis=0, keepdims=True)
        weight = jnp.exp2((scores - top) * score_mul)
        wsum = jnp.sum(weight, axis=0, keepdims=True)
        value = lax.dot_general(weight.astype(BF16), qkv[1], CONTRACT_FIRST, preferred_element_type=F32)[:16]
        diag = lax.broadcasted_iota(jnp.int32, (16, 128), 0) == lax.broadcasted_iota(jnp.int32, (16, 128), 1)
        wcol = jnp.sum(jnp.where(diag, jnp.broadcast_to(wsum, (16, 128)), 0.0), axis=1, keepdims=True)
        pooled = jnp.sum(jnp.where(own_head, value / wcol, 0.0), axis=0, keepdims=True)
        abuf[pl.ds(img, 1), :] = pooled
        return carry

    lax.fori_loop(0, own, one_image, 0)

    load(6).wait()
    load(7).wait()
    load(8).wait()
    pooled_out = (dot(abuf[...].astype(BF16), wout[...]) + vrow(V_PBOUT)).astype(BF16).astype(F32)
    normed_out = layer_norm(pooled_out, vrow(V_PLNS), vrow(V_PLNB)).astype(BF16)
    total = pooled_out + vrow(V_PBDOWN)
    for c in range(4):
        up = dot(normed_out, wup[:, c * 1024:(c + 1) * 1024]) + vrow(V_PBUP + c)
        total = total + dot(gelu(up).astype(BF16), wdown[c])
    emb[...] = total[:8]

    def drain(img, carry):
        for step in range(1, group):
            piece(img, step).wait_send()
        return carry

    lax.fori_loop(0, own, drain, 0)

    def share(step):
        return pltpu.make_async_remote_copy(
            src_ref=emb, dst_ref=gath.at[me], send_sem=gsend_sem.at[step], recv_sem=grecv_sem.at[me],
            device_id={"cp": peer(step)}, device_id_type=MESH)

    for step in range(1, group):
        share(step).start()
    gath[me] = emb[...]
    for step in range(1, group):
        src = lax.rem(me + step, group)
        pltpu.make_async_copy(emb, gath.at[src], grecv_sem.at[src]).wait()
    for step in range(1, group):
        share(step).wait_send()
    for src in range(group):
        out_ref[src * own:(src + 1) * own, :] = gath[src][:own]


def solution(mesh):
    group = mesh.shape["cp"]

    def device_step(images, ln1_scale, ln1_bias, w_qkv, b_qkv, w_out, b_out, ln2_scale, ln2_bias, w_up, b_up, w_down, b_down, lnf_scale, lnf_bias, pool_probe, pool_wq, pool_bq, pool_wkv, pool_bkv, pool_wout, pool_bout, pool_ln_scale, pool_ln_bias, pool_w_up, pool_b_up, pool_w_down, pool_b_down):
        n_img, run, width = images.shape
        own = n_img // group
        rows = group * run
        vec = jnp.concatenate([v.reshape(-1) for v in (
            ln1_scale, ln1_bias, b_qkv, b_out, ln2_scale, ln2_bias, b_up, b_down, lnf_scale, lnf_bias, pool_bq, pool_bkv,
            pool_bout, pool_ln_scale, pool_ln_bias, pool_b_up, pool_b_down)]).reshape(V_ROWS, width)
        wqkv = w_qkv.transpose(1, 2, 3, 0).reshape(3, width, width)
        pwq = pool_wq.transpose(1, 2, 0).reshape(width, width)
        pwkv = pool_wkv.transpose(1, 2, 3, 0).reshape(2, width, width)
        any_spec = pl.BlockSpec(memory_space=pl.ANY)
        vmem_spec = pl.BlockSpec(memory_space=pltpu.VMEM)
        return pl.pallas_call(
            functools.partial(kernel, group, own, run),
            out_shape=jax.ShapeDtypeStruct((n_img, width), F32),
            in_specs=[any_spec, vmem_spec, vmem_spec] + [any_spec] * 9,
            out_specs=vmem_spec,
            scratch_shapes=[
                pltpu.VMEM((own, group, run, width), BF16),
                pltpu.VMEM((3, width, width), BF16),
                pltpu.VMEM((width, width), BF16),
                pltpu.VMEM((width, 4 * width), BF16),
                pltpu.VMEM((4, width, width), BF16),
                pltpu.VMEM((width, width), BF16),
                pltpu.VMEM((2, width, width), BF16),
                pltpu.VMEM((rows, width), BF16),
                pltpu.VMEM((3, rows, width), BF16),
                pltpu.VMEM((rows, width), BF16),
                pltpu.VMEM((rows, width), BF16),
                pltpu.VMEM((rows, width), BF16),
                pltpu.VMEM((rows, width), F32),
                pltpu.VMEM((128, width), BF16),
                pltpu.VMEM((16, width), F32),
                pltpu.VMEM((8, width), F32),
                pltpu.VMEM((group, 8, width), F32),
                pltpu.SemaphoreType.DMA((own, group)),
                pltpu.SemaphoreType.DMA((own, group)),
                pltpu.SemaphoreType.DMA((9,)),
                pltpu.SemaphoreType.DMA((group,)),
                pltpu.SemaphoreType.DMA((group,)),
            ],
            compiler_params=pltpu.CompilerParams(collective_id=0, has_side_effects=True, vmem_limit_bytes=67043328),
        )(images, vec, pool_probe, wqkv, w_out.reshape(width, width), w_up, w_down.reshape(4, width, width), pwq, pwkv,
          pool_wout.reshape(width, width), pool_w_up, pool_w_down.reshape(4, width, width))

    in_specs = (P("dp", "cp", None),) + (P(),) * 27
    return jax.shard_map(device_step, mesh=mesh, in_specs=in_specs, out_specs=P("dp", None), check_vma=False)
```

```python
import functools

import jax
import jax.numpy as jnp
from jax import lax
from jax.experimental import pallas as pl
from jax.experimental.pallas import tpu as pltpu
from jax.sharding import PartitionSpec as P

EPSILON = 1e-6
MESH = pl.DeviceIdType.MESH
BF16 = jnp.bfloat16
F32 = jnp.float32
LOG2E = 1.4426950408889634
CONTRACT_LAST = (((1,), (1,)), ((), ()))
CONTRACT_FIRST = (((0,), (0,)), ((), ()))

def layer_norm(values, ln_gain, ln_shift):
    row_mean = jnp.mean(values, axis=-1, keepdims=True)
    centered = values - row_mean
    variance = jnp.mean(centered * centered, axis=-1, keepdims=True)
    return centered * lax.rsqrt(variance + EPSILON) * ln_gain + ln_shift


def gelu(x):
    c0 = 0.7978845608028654
    return (0.5 * x) * (1.0 + jnp.tanh(x * (c0 + (c0 * 0.044715) * (x * x))))


def dot_t(lhs, rhs):
    return lax.dot_general(lhs, rhs, CONTRACT_LAST, preferred_element_type=F32)


def dot(lhs, rhs):
    return jnp.dot(lhs, rhs, preferred_element_type=F32)


def kernel(group, own, run, images, ln1s, ln1b, bqkv_in, bout, ln2s, ln2b, bup, bdown, lnfs, lnfb, pbq_in, pbkv_in, pbout, plns, plnb, pbup, pbdown,
           probe, wqkv_hbm, wout_hbm, wup_hbm, wdown_hbm, pwq_hbm, pwkv_hbm, pwout_hbm, pwup_hbm, pwdown_hbm,
           out_ref, xbuf, wqkv, wout, wup, wdown, pwq, pwkv, hbuf, qkv, ctx, rbuf, mbuf, acc, ublk, bias, abuf, emb, gath,
           send_sem, recv_sem, w_sem, gsend_sem, grecv_sem):
    me = lax.axis_index("cp")
    width = 1024
    rows = group * run
    pair = 2 * run
    n_pair = group // 2

    def peer(step):
        return lax.rem(me + step, group)

    weights = ((wqkv_hbm, wqkv), (pwq_hbm, pwq), (wout_hbm, wout), (wup_hbm, wup), (wdown_hbm, wdown), (pwkv_hbm, pwkv),
               (pwout_hbm, wout), (pwup_hbm, wup), (pwdown_hbm, wdown))

    def load(k):
        return pltpu.make_async_copy(weights[k][0], weights[k][1], w_sem.at[k])

    def piece(img, step):
        dst = peer(step)
        return pltpu.make_async_remote_copy(
            src_ref=images.at[dst * own + img], dst_ref=xbuf.at[img, me],
            send_sem=send_sem.at[img, step], recv_sem=recv_sem.at[img, me],
            device_id={"cp": dst}, device_id_type=MESH)

    def local_piece(img):
        return pltpu.make_async_copy(images.at[me * own + img], xbuf.at[img, me], recv_sem.at[img, me])

    load(0).start()
    load(1).start()
    barrier = pltpu.get_barrier_semaphore()
    for step in range(1, group):
        pl.semaphore_signal(barrier, inc=1, device_id={"cp": peer(step)}, device_id_type=MESH)
    pl.semaphore_wait(barrier, group - 1)

    def send_image(img, carry):
        local_piece(img).start()
        for step in (6, 2, 4, 7, 3, 5, 1):
            piece(img, step).start()
        return carry

    send_image(0, 0)
    for k in range(2, 6):
        load(k).start()

    for row, (ref, at) in enumerate(((bqkv_in, 0), (bqkv_in, 1), (bqkv_in, 2), (pbkv_in, 0), (pbkv_in, 1), (pbq_in, 0))):
        table = ref[at]
        bias[row:row + 1, :] = jnp.concatenate([table[h:h + 1, :] for h in range(16)], axis=1)

    load(1).wait()
    probe_rows = jnp.broadcast_to(probe[...], (16, width))
    u = (dot_t(probe_rows, pwq[...]) + bias[5:6, :]).astype(BF16).astype(F32)
    head_of_lane = lax.broadcasted_iota(jnp.int32, (16, width), 1) // 64
    head_of_row = lax.broadcasted_iota(jnp.int32, (16, width), 0)
    own_head = head_of_lane == head_of_row
    ublk[...] = jnp.concatenate([jnp.where(own_head, u, 0.0), jnp.zeros((112, width), F32)], axis=0).astype(BF16)
    abuf[...] = jnp.zeros_like(abuf)

    def x_pair(img, pp):
        return jnp.concatenate([xbuf[img, 2 * pp].astype(F32), xbuf[img, 2 * pp + 1].astype(F32)], axis=0)

    def one_image(img, carry):
        first = img == 0
        last = img == own - 1

        for src in range(group):
            pltpu.make_async_copy(images.at[0], xbuf.at[img, src], recv_sem.at[img, src]).wait()

        @pl.when(img + 1 < own)
        def _():
            send_image(img + 1, 0)

        for pp in range(n_pair):
            hbuf[pl.ds(pp * pair, pair), :] = layer_norm(x_pair(img, pp), ln1s[...], ln1b[...]).astype(BF16)

        @pl.when(first)
        def _():
            load(0).wait()

        def project(c, carry):
            qkv[c] = (dot_t(hbuf[...], wqkv[c]) + bias[pl.ds(c, 1), :]).astype(BF16)
            return carry

        lax.fori_loop(0, 3, project, 0)

        lane = lax.broadcasted_iota(jnp.int32, (1, 128), 1)
        low = (lane < 64).astype(F32)
        low_b = low.astype(BF16)
        high_b = (1.0 - low).astype(BF16)
        score_mul = LOG2E * 0.125

        def head_pair(hp, carry):
            cols = pl.ds(pl.multiple_of(hp * 128, 128), 128)
            q2, k2, v2 = qkv[0, :, cols], qkv[1, :, cols], qkv[2, :, cols]

            def soft(q_half):
                scores = dot_t(q_half, k2)
                top = jnp.max(scores, axis=-1, keepdims=True)
                weight = jnp.exp2((scores - top) * score_mul)
                return weight.astype(BF16), jnp.sum(weight, axis=-1, keepdims=True)

            w_lo, l_lo = soft(q2 * low_b)
            w_hi, l_hi = soft(q2 * high_b)
            total = dot(w_lo, v2 * low_b) + dot(w_hi, v2 * high_b)
            denom = jnp.where(lane < 64, l_lo, l_hi)
            ctx[:, cols] = (total / denom).astype(BF16)
            return carry

        lax.fori_loop(0, 8, head_pair, 0)

        @pl.when(first)
        def _():
            load(2).wait()

        acc[...] = dot(ctx[...], wout[...])

        @pl.when(last)
        def _():
            load(6).start()

        for pp in range(n_pair):
            block = pl.ds(pp * pair, pair)
            r = (x_pair(img, pp) + (acc[block, :] + bout[...])).astype(BF16)
            rbuf[block, :] = r
            hbuf[block, :] = layer_norm(r.astype(F32), ln2s[...], ln2b[...]).astype(BF16)

        @pl.when(first)
        def _():
            load(3).wait()
            load(4).wait()

        acc[...] = rbuf[...].astype(F32) + bdown[...]

        def hidden_chunk(c, carry):
            cols = pl.ds(pl.multiple_of(c * 1024, 1024), 1024)
            up = dot(hbuf[...], wup[:, cols]) + bup[:, cols]
            mbuf[...] = gelu(up).astype(BF16)
            acc[...] += dot(mbuf[...], wdown[c])
            return carry

        lax.fori_loop(0, 4, hidden_chunk, 0)

        @pl.when(last)
        def _():
            load(7).start()
            load(8).start()

        for pp in range(n_pair):
            block = pl.ds(pp * pair, pair)
            y = acc[block, :].astype(BF16).astype(F32)
            hbuf[block, :] = layer_norm(y, lnfs[...], lnfb[...]).astype(BF16)

        @pl.when(first)
        def _():
            load(5).wait()

        def pool_project(c, carry):
            qkv[c] = (dot_t(hbuf[...], pwkv[c]) + bias[pl.ds(3 + c, 1), :]).astype(BF16)
            return carry

        lax.fori_loop(0, 2, pool_project, 0)
        scores = dot_t(qkv[0], ublk[...])
        top = jnp.max(scores, axis=0, keepdims=True)
        weight = jnp.exp2((scores - top) * score_mul)
        wsum = jnp.sum(weight, axis=0, keepdims=True)
        value = lax.dot_general(weight.astype(BF16), qkv[1], CONTRACT_FIRST, preferred_element_type=F32)[:16]
        diag = lax.broadcasted_iota(jnp.int32, (16, 128), 0) == lax.broadcasted_iota(jnp.int32, (16, 128), 1)
        wcol = jnp.sum(jnp.where(diag, jnp.broadcast_to(wsum, (16, 128)), 0.0), axis=1, keepdims=True)
        pooled = jnp.sum(jnp.where(own_head, value / wcol, 0.0), axis=0, keepdims=True)
        abuf[pl.ds(img, 1), :] = pooled
        return carry

    lax.fori_loop(0, own, one_image, 0)

    load(6).wait()
    load(7).wait()
    load(8).wait()
    pooled_out = (dot(abuf[...].astype(BF16), wout[...]) + pbout[...]).astype(BF16).astype(F32)
    normed_out = layer_norm(pooled_out, plns[...], plnb[...]).astype(BF16)
    total = pooled_out + pbdown[...]
    for c in range(4):
        up = dot(normed_out, wup[:, c * 1024:(c + 1) * 1024]) + pbup[:, c * 1024:(c + 1) * 1024]
        total = total + dot(gelu(up).astype(BF16), wdown[c])
    emb[...] = total[:8]

    def drain(img, carry):
        for step in range(1, group):
            piece(img, step).wait_send()
        return carry

    lax.fori_loop(0, own, drain, 0)

    def share(step):
        return pltpu.make_async_remote_copy(
            src_ref=emb, dst_ref=gath.at[me], send_sem=gsend_sem.at[step], recv_sem=grecv_sem.at[me],
            device_id={"cp": peer(step)}, device_id_type=MESH)

    for step in range(1, group):
        share(step).start()
    gath[me] = emb[...]
    for step in range(1, group):
        src = lax.rem(me + step, group)
        pltpu.make_async_copy(emb, gath.at[src], grecv_sem.at[src]).wait()
    for step in range(1, group):
        share(step).wait_send()
    for src in range(group):
        out_ref[src * own:(src + 1) * own, :] = gath[src][:own]


def solution(mesh):
    group = mesh.shape["cp"]

    def device_step(images, ln1_scale, ln1_bias, w_qkv, b_qkv, w_out, b_out, ln2_scale, ln2_bias, w_up, b_up, w_down, b_down, lnf_scale, lnf_bias, pool_probe, pool_wq, pool_bq, pool_wkv, pool_bkv, pool_wout, pool_bout, pool_ln_scale, pool_ln_bias, pool_w_up, pool_b_up, pool_w_down, pool_b_down):
        n_img, run, width = images.shape
        own = n_img // group
        rows = group * run
        row = lambda v: v.reshape(1, -1)
        wqkv = w_qkv.transpose(1, 2, 3, 0).reshape(3, width, width)
        pwq = pool_wq.transpose(1, 2, 0).reshape(width, width)
        pwkv = pool_wkv.transpose(1, 2, 3, 0).reshape(2, width, width)
        any_spec = pl.BlockSpec(memory_space=pl.ANY)
        vmem_spec = pl.BlockSpec(memory_space=pltpu.VMEM)
        return pl.pallas_call(
            functools.partial(kernel, group, own, run),
            out_shape=jax.ShapeDtypeStruct((n_img, width), F32),
            in_specs=[any_spec] + [vmem_spec] * 18 + [any_spec] * 9,
            out_specs=vmem_spec,
            scratch_shapes=[
                pltpu.VMEM((own, group, run, width), BF16),
                pltpu.VMEM((3, width, width), BF16),
                pltpu.VMEM((width, width), BF16),
                pltpu.VMEM((width, 4 * width), BF16),
                pltpu.VMEM((4, width, width), BF16),
                pltpu.VMEM((width, width), BF16),
                pltpu.VMEM((2, width, width), BF16),
                pltpu.VMEM((rows, width), BF16),
                pltpu.VMEM((3, rows, width), BF16),
                pltpu.VMEM((rows, width), BF16),
                pltpu.VMEM((rows, width), BF16),
                pltpu.VMEM((rows, width), BF16),
                pltpu.VMEM((rows, width), F32),
                pltpu.VMEM((128, width), BF16),
                pltpu.VMEM((8, width), F32),
                pltpu.VMEM((16, width), F32),
                pltpu.VMEM((8, width), F32),
                pltpu.VMEM((group, 8, width), F32),
                pltpu.SemaphoreType.DMA((own, group)),
                pltpu.SemaphoreType.DMA((own, group)),
                pltpu.SemaphoreType.DMA((9,)),
                pltpu.SemaphoreType.DMA((group,)),
                pltpu.SemaphoreType.DMA((group,)),
            ],
            compiler_params=pltpu.CompilerParams(collective_id=0, has_side_effects=True, vmem_limit_bytes=67043328),
        )(images, row(ln1_scale), row(ln1_bias), b_qkv, row(b_out), row(ln2_scale), row(ln2_bias), row(b_up), row(b_down),
          row(lnf_scale), row(lnf_bias), pool_bq[None], pool_bkv, row(pool_bout), row(pool_ln_scale), row(pool_ln_bias),
          row(pool_b_up), row(pool_b_down), pool_probe, wqkv, w_out.reshape(width, width), w_up, w_down.reshape(4, width, width), pwq, pwkv,
          pool_wout.reshape(width, width), pool_w_up, pool_w_down.reshape(4, width, width))

    in_specs = (P("dp", "cp", None),) + (P(),) * 27
    return jax.shard_map(device_step, mesh=mesh, in_specs=in_specs, out_specs=P("dp", None), check_vma=False)
```

```python
import functools

import jax
import jax.numpy as jnp
from jax import lax
from jax.experimental import pallas as pl
from jax.experimental.pallas import tpu as pltpu
from jax.sharding import PartitionSpec as P

EPSILON = 1e-6
MESH = pl.DeviceIdType.MESH
BF16 = jnp.bfloat16
F32 = jnp.float32
LOG2E = 1.4426950408889634
CONTRACT_LAST = (((1,), (1,)), ((), ()))
CONTRACT_FIRST = (((0,), (0,)), ((), ()))

def layer_norm(values, ln_gain, ln_shift):
    row_mean = jnp.mean(values, axis=-1, keepdims=True)
    centered = values - row_mean
    variance = jnp.mean(centered * centered, axis=-1, keepdims=True)
    return centered * lax.rsqrt(variance + EPSILON) * ln_gain + ln_shift


def gelu(x):
    c0 = 0.7978845608028654
    return (0.5 * x) * (1.0 + jnp.tanh(x * (c0 + (c0 * 0.044715) * (x * x))))


def dot_t(lhs, rhs):
    return lax.dot_general(lhs, rhs, CONTRACT_LAST, preferred_element_type=F32)


def dot(lhs, rhs):
    return jnp.dot(lhs, rhs, preferred_element_type=F32)


def blocks(ref, count, first=0, rows=slice(None)):
    return jnp.concatenate([ref[first + c, rows, :] for c in range(count)], axis=1)


def put(ref, value, count, first=0, rows=slice(None)):
    for c in range(count):
        ref[first + c, rows, :] = value[:, c * 128:(c + 1) * 128].astype(BF16)


def kernel(group, own, run, images, ln1s, ln1b, bqkv_in, bout, ln2s, ln2b, bup, bdown, lnfs, lnfb, pbq_in, pbkv_in, pbout, plns, plnb, pbup, pbdown,
           probe, wqkv_hbm, wout_hbm, wup_hbm, wdown_hbm, pwq_hbm, pwkv_hbm, pwout_hbm, pwup_hbm, pwdown_hbm,
           out_ref, xbuf, wqkv, wout, wup, wdown, pwkv, hbuf, qkv, ctx, mbuf, acc, ublk, bias, abuf, emb, gath,
           send_sem, recv_sem, w_sem, gsend_sem, grecv_sem):
    me = lax.axis_index("cp")
    width = 1024
    rows = group * run

    def peer(step):
        return lax.rem(me + step, group)

    weights = ((wqkv_hbm, wqkv), (pwq_hbm, pwkv.at[:, :width]), (wout_hbm, wout), (wup_hbm, wup), (wdown_hbm, wdown), (pwkv_hbm, pwkv),
               (pwout_hbm, wout), (pwup_hbm, wup), (pwdown_hbm, wdown))

    def start(k):
        src, dst = weights[k]

        def one(c, carry):
            cols = pl.ds(pl.multiple_of(c * 128, 128), 128)
            pltpu.make_async_copy(src.at[:, cols], dst.at[c], w_sem.at[k]).start()
            return carry

        lax.fori_loop(0, src.shape[1] // 128, one, 0)

    def arrived(k):
        dst = weights[k][1]
        pltpu.make_async_copy(dst, dst, w_sem.at[k]).wait()

    def piece(img, step):
        dst = peer(step)
        return pltpu.make_async_remote_copy(
            src_ref=images.at[dst * own + img], dst_ref=xbuf.at[img, me],
            send_sem=send_sem.at[img, step], recv_sem=recv_sem.at[img, me],
            device_id={"cp": dst}, device_id_type=MESH)

    def local_piece(img):
        return pltpu.make_async_copy(images.at[me * own + img], xbuf.at[img, me], recv_sem.at[img, me])

    start(0)
    start(1)
    barrier = pltpu.get_barrier_semaphore()
    for step in range(1, group):
        pl.semaphore_signal(barrier, inc=1, device_id={"cp": peer(step)}, device_id_type=MESH)
    pl.semaphore_wait(barrier, group - 1)

    def send_image(img, carry):
        local_piece(img).start()
        for step in (6, 2, 4, 7, 3, 5, 1):
            piece(img, step).start()
        return carry

    send_image(0, 0)
    for k in range(2, 5):
        start(k)

    for row, (ref, at) in enumerate(((bqkv_in, 0), (bqkv_in, 1), (bqkv_in, 2), (pbkv_in, 0), (pbkv_in, 1), (pbq_in, 0))):
        table = ref[at]
        bias[row:row + 1, :] = jnp.concatenate([table[h:h + 1, :] for h in range(16)], axis=1)

    arrived(1)
    probe_rows = jnp.broadcast_to(probe[...], (16, width))
    u = (dot_t(probe_rows, blocks(pwkv, 8, rows=slice(0, width))) + bias[5:6, :]).astype(BF16).astype(F32)
    head_of_lane = lax.broadcasted_iota(jnp.int32, (16, width), 1) // 64
    head_of_row = lax.broadcasted_iota(jnp.int32, (16, width), 0)
    own_head = head_of_lane == head_of_row
    put(ublk, jnp.concatenate([jnp.where(own_head, u, 0.0), jnp.zeros((112, width), F32)], axis=0), 8)
    start(5)
    abuf[...] = jnp.zeros_like(abuf)

    chunk = 16

    def x_rows(img, at):
        src, off = at // run, at % run
        if off + chunk <= run:
            return xbuf[img, src, off:off + chunk].astype(F32)
        return jnp.concatenate([xbuf[img, src, off:].astype(F32), xbuf[img, src + 1, :off + chunk - run].astype(F32)], axis=0)

    def one_image(img, carry):
        first = img == 0
        last = img == own - 1

        for src in range(group):
            pltpu.make_async_copy(images.at[0], xbuf.at[img, src], recv_sem.at[img, src]).wait()

        @pl.when(img + 1 < own)
        def _():
            send_image(img + 1, 0)

        for at in range(0, rows, chunk):
            put(hbuf, layer_norm(x_rows(img, at), ln1s[...], ln1b[...]), 8, rows=slice(at, at + chunk))

        @pl.when(first)
        def _():
            arrived(0)

        def project(c, carry):
            weight = blocks(wqkv, 8, rows=pl.ds(pl.multiple_of(c * width, width), width))
            put(qkv, dot_t(blocks(hbuf, 8), weight) + bias[pl.ds(c, 1), :], 8, first=c * 8)
            return carry

        lax.fori_loop(0, 3, project, 0)

        lane = lax.broadcasted_iota(jnp.int32, (1, 128), 1)
        low = (lane < 64).astype(F32)
        low_b = low.astype(BF16)
        high_b = (1.0 - low).astype(BF16)
        score_mul = LOG2E * 0.125

        def head_pair(hp, carry):
            q2, k2, v2 = qkv[hp], qkv[8 + hp], qkv[16 + hp]

            def soft(q_half):
                scores = dot_t(q_half, k2)
                top = jnp.max(scores, axis=-1, keepdims=True)
                weight = jnp.exp2((scores - top) * score_mul)
                return weight.astype(BF16), jnp.sum(weight, axis=-1, keepdims=True)

            w_lo, l_lo = soft(q2 * low_b)
            w_hi, l_hi = soft(q2 * high_b)
            total = dot(w_lo, v2 * low_b) + dot(w_hi, v2 * high_b)
            denom = jnp.where(lane < 64, l_lo, l_hi)
            ctx[hp] = (total / denom).astype(BF16)
            return carry

        lax.fori_loop(0, 8, head_pair, 0)

        @pl.when(first)
        def _():
            arrived(2)

        acc[...] = dot(blocks(ctx, 8), blocks(wout, 8))

        @pl.when(last)
        def _():
            start(6)

        for at in range(0, rows, chunk):
            block = slice(at, at + chunk)
            r = (x_rows(img, at) + (acc[block, :] + bout[...])).astype(BF16).astype(F32)
            acc[block, :] = r + bdown[...]
            put(hbuf, layer_norm(r, ln2s[...], ln2b[...]), 8, rows=block)

        @pl.when(first)
        def _():
            arrived(3)
            arrived(4)

        def hidden_chunk(c, carry):
            cols = pl.ds(pl.multiple_of(c * width, width), width)
            put(mbuf, gelu(dot(blocks(hbuf, 8), blocks(wup, 8, first=c * 8)) + bup[:, cols]), 8)
            acc[...] += dot(blocks(mbuf, 8), blocks(wdown, 8, rows=cols))
            return carry

        lax.fori_loop(0, 4, hidden_chunk, 0)

        @pl.when(last)
        def _():
            start(7)
            start(8)

        for at in range(0, rows, chunk):
            block = slice(at, at + chunk)
            y = acc[block, :].astype(BF16).astype(F32)
            put(hbuf, layer_norm(y, lnfs[...], lnfb[...]), 8, rows=block)

        @pl.when(first)
        def _():
            arrived(5)

        for c in range(2):
            weight = blocks(pwkv, 8, rows=slice(c * width, (c + 1) * width))
            put(qkv, dot_t(blocks(hbuf, 8), weight) + bias[3 + c:4 + c, :], 8, first=c * 8)
        scores = dot_t(blocks(qkv, 8), blocks(ublk, 8))
        top = jnp.max(scores, axis=0, keepdims=True)
        weight = jnp.exp2((scores - top) * score_mul)
        wsum = jnp.sum(weight, axis=0, keepdims=True)
        value = lax.dot_general(weight.astype(BF16), blocks(qkv, 8, first=8), CONTRACT_FIRST, preferred_element_type=F32)[:16]
        diag = lax.broadcasted_iota(jnp.int32, (16, 128), 0) == lax.broadcasted_iota(jnp.int32, (16, 128), 1)
        wcol = jnp.sum(jnp.where(diag, jnp.broadcast_to(wsum, (16, 128)), 0.0), axis=1, keepdims=True)
        pooled = jnp.sum(jnp.where(own_head, value / wcol, 0.0), axis=0, keepdims=True)
        abuf[pl.ds(img, 1), :] = pooled
        return carry

    lax.fori_loop(0, own, one_image, 0)

    arrived(6)
    arrived(7)
    arrived(8)
    pooled_out = (dot(abuf[...].astype(BF16), blocks(wout, 8)) + pbout[...]).astype(BF16).astype(F32)
    normed_out = layer_norm(pooled_out, plns[...], plnb[...]).astype(BF16)
    total = pooled_out + pbdown[...]
    for c in range(4):
        up = dot(normed_out, blocks(wup, 8, first=c * 8)) + pbup[:, c * 1024:(c + 1) * 1024]
        total = total + dot(gelu(up).astype(BF16), blocks(wdown, 8, rows=slice(c * 1024, (c + 1) * 1024)))
    emb[...] = total[:8]

    def drain(img, carry):
        for step in range(1, group):
            piece(img, step).wait_send()
        return carry

    lax.fori_loop(0, own, drain, 0)

    def share(step):
        return pltpu.make_async_remote_copy(
            src_ref=emb, dst_ref=gath.at[me], send_sem=gsend_sem.at[step], recv_sem=grecv_sem.at[me],
            device_id={"cp": peer(step)}, device_id_type=MESH)

    for step in range(1, group):
        share(step).start()
    gath[me] = emb[...]
    for step in range(1, group):
        src = lax.rem(me + step, group)
        pltpu.make_async_copy(emb, gath.at[src], grecv_sem.at[src]).wait()
    for step in range(1, group):
        share(step).wait_send()
    for src in range(group):
        out_ref[src * own:(src + 1) * own, :] = gath[src][:own]


def solution(mesh):
    group = mesh.shape["cp"]

    def device_step(images, ln1_scale, ln1_bias, w_qkv, b_qkv, w_out, b_out, ln2_scale, ln2_bias, w_up, b_up, w_down, b_down, lnf_scale, lnf_bias, pool_probe, pool_wq, pool_bq, pool_wkv, pool_bkv, pool_wout, pool_bout, pool_ln_scale, pool_ln_bias, pool_w_up, pool_b_up, pool_w_down, pool_b_down):
        n_img, run, width = images.shape
        own = n_img // group
        rows = group * run
        row = lambda v: v.reshape(1, -1)
        wqkv = w_qkv.transpose(1, 2, 3, 0).reshape(3 * width, width)
        pwq = pool_wq.transpose(1, 2, 0).reshape(width, width)
        pwkv = pool_wkv.transpose(1, 2, 3, 0).reshape(2 * width, width)
        any_spec = pl.BlockSpec(memory_space=pl.ANY)
        vmem_spec = pl.BlockSpec(memory_space=pltpu.VMEM)
        return pl.pallas_call(
            functools.partial(kernel, group, own, run),
            out_shape=jax.ShapeDtypeStruct((n_img, width), F32),
            in_specs=[any_spec] + [vmem_spec] * 18 + [any_spec] * 9,
            out_specs=vmem_spec,
            scratch_shapes=[
                pltpu.VMEM((own, group, run, width), BF16),
                pltpu.VMEM((8, 3 * width, 128), BF16),
                pltpu.VMEM((8, width, 128), BF16),
                pltpu.VMEM((32, width, 128), BF16),
                pltpu.VMEM((8, 4 * width, 128), BF16),
                pltpu.VMEM((8, 2 * width, 128), BF16),
                pltpu.VMEM((8, rows, 128), BF16),
                pltpu.VMEM((24, rows, 128), BF16),
                pltpu.VMEM((8, rows, 128), BF16),
                pltpu.VMEM((8, rows, 128), BF16),
                pltpu.VMEM((rows, width), F32),
                pltpu.VMEM((8, 128, 128), BF16),
                pltpu.VMEM((8, width), F32),
                pltpu.VMEM((16, width), F32),
                pltpu.VMEM((8, width), F32),
                pltpu.VMEM((group, 8, width), F32),
                pltpu.SemaphoreType.DMA((own, group)),
                pltpu.SemaphoreType.DMA((own, group)),
                pltpu.SemaphoreType.DMA((9,)),
                pltpu.SemaphoreType.DMA((group,)),
                pltpu.SemaphoreType.DMA((group,)),
            ],
            compiler_params=pltpu.CompilerParams(collective_id=0, has_side_effects=True, vmem_limit_bytes=67043328),
        )(images, row(ln1_scale), row(ln1_bias), b_qkv, row(b_out), row(ln2_scale), row(ln2_bias), row(b_up), row(b_down),
          row(lnf_scale), row(lnf_bias), pool_bq[None], pool_bkv, row(pool_bout), row(pool_ln_scale), row(pool_ln_bias),
          row(pool_b_up), row(pool_b_down), pool_probe, wqkv, w_out.reshape(width, width), w_up, w_down, pwq, pwkv,
          pool_wout.reshape(width, width), pool_w_up, pool_w_down)

    in_specs = (P("dp", "cp", None),) + (P(),) * 27
    return jax.shard_map(device_step, mesh=mesh, in_specs=in_specs, out_specs=P("dp", None), check_vma=False)
```

```python
import functools

import jax
import jax.numpy as jnp
from jax import lax
from jax.experimental import pallas as pl
from jax.experimental.pallas import tpu as pltpu
from jax.sharding import PartitionSpec as P

EPSILON = 1e-6
MESH = pl.DeviceIdType.MESH
BF16 = jnp.bfloat16
F32 = jnp.float32
LOG2E = 1.4426950408889634
CONTRACT_LAST = (((1,), (1,)), ((), ()))
CONTRACT_FIRST = (((0,), (0,)), ((), ()))

def layer_norm(values, ln_gain, ln_shift):
    row_mean = jnp.mean(values, axis=-1, keepdims=True)
    centered = values - row_mean
    variance = jnp.mean(centered * centered, axis=-1, keepdims=True)
    return centered * lax.rsqrt(variance + EPSILON) * ln_gain + ln_shift


def gelu(x):
    c0 = 0.7978845608028654
    return (0.5 * x) * (1.0 + jnp.tanh(x * (c0 + (c0 * 0.044715) * (x * x))))


def dot_t(lhs, rhs):
    return lax.dot_general(lhs, rhs, CONTRACT_LAST, preferred_element_type=F32)


def dot(lhs, rhs):
    return jnp.dot(lhs, rhs, preferred_element_type=F32)


def blocks(ref, count, first=0, rows=slice(None)):
    return jnp.concatenate([ref[first + c, rows, :] for c in range(count)], axis=1)


def put(ref, value, count, first=0, rows=slice(None)):
    for c in range(count):
        ref[first + c, rows, :] = value[:, c * 128:(c + 1) * 128].astype(BF16)


def kernel(group, own, run, images, ln1s, ln1b, bqkv_in, bout, ln2s, ln2b, bup, bdown, lnfs, lnfb, pbq_in, pbkv_in, pbout, plns, plnb, pbup, pbdown,
           probe, wqkv_hbm, wout_hbm, wup_hbm, wdown_hbm, pwq_hbm, pwkv_hbm, pwout_hbm, pwup_hbm, pwdown_hbm,
           out_ref, xbuf, wqkv, wout, wup, wdown, pwkv, hbuf, qkv, ctx, mbuf, acc, ublk, bias, abuf, emb, gath,
           send_sem, recv_sem, w_sem, gsend_sem, grecv_sem):
    me = lax.axis_index("cp")
    width = 1024
    rows = group * run

    def peer(step):
        return lax.rem(me + step, group)

    weights = ((wqkv_hbm, wqkv), (pwq_hbm, pwkv.at[:, :width]), (wout_hbm, wout), (wup_hbm, wup), (wdown_hbm, wdown), (pwkv_hbm, pwkv),
               (pwout_hbm, wout), (pwup_hbm, wup), (pwdown_hbm, wdown))

    def start(k):
        src, dst = weights[k]

        def one(c, carry):
            cols = pl.ds(pl.multiple_of(c * 512, 512), 512)
            pltpu.make_async_copy(src.at[:, cols], dst.at[c], w_sem.at[k]).start()
            return carry

        lax.fori_loop(0, src.shape[1] // 512, one, 0)

    def arrived(k):
        dst = weights[k][1]
        pltpu.make_async_copy(dst, dst, w_sem.at[k]).wait()

    def piece(img, step):
        dst = peer(step)
        return pltpu.make_async_remote_copy(
            src_ref=images.at[dst * own + img], dst_ref=xbuf.at[img, me],
            send_sem=send_sem.at[img, step], recv_sem=recv_sem.at[img, me],
            device_id={"cp": dst}, device_id_type=MESH)

    def local_piece(img):
        return pltpu.make_async_copy(images.at[me * own + img], xbuf.at[img, me], recv_sem.at[img, me])

    start(0)
    start(1)
    barrier = pltpu.get_barrier_semaphore()
    for step in range(1, group):
        pl.semaphore_signal(barrier, inc=1, device_id={"cp": peer(step)}, device_id_type=MESH)
    pl.semaphore_wait(barrier, group - 1)

    def send_image(img, carry):
        local_piece(img).start()
        for step in (6, 2, 4, 7, 3, 5, 1):
            piece(img, step).start()
        return carry

    send_image(0, 0)
    for k in range(2, 5):
        start(k)

    for row, (ref, at) in enumerate(((bqkv_in, 0), (bqkv_in, 1), (bqkv_in, 2), (pbkv_in, 0), (pbkv_in, 1), (pbq_in, 0))):
        table = ref[at]
        bias[row:row + 1, :] = jnp.concatenate([table[h:h + 1, :] for h in range(16)], axis=1)

    arrived(1)
    probe_rows = jnp.broadcast_to(probe[...], (16, width))
    u = (dot_t(probe_rows, blocks(pwkv, 2, rows=slice(0, width))) + bias[5:6, :]).astype(BF16).astype(F32)
    head_of_lane = lax.broadcasted_iota(jnp.int32, (16, width), 1) // 64
    head_of_row = lax.broadcasted_iota(jnp.int32, (16, width), 0)
    own_head = head_of_lane == head_of_row
    put(ublk, jnp.concatenate([jnp.where(own_head, u, 0.0), jnp.zeros((112, width), F32)], axis=0), 8)
    start(5)
    abuf[...] = jnp.zeros_like(abuf)

    chunk = 16

    def x_rows(img, at):
        src, off = at // run, at % run
        if off + chunk <= run:
            return xbuf[img, src, off:off + chunk].astype(F32)
        return jnp.concatenate([xbuf[img, src, off:].astype(F32), xbuf[img, src + 1, :off + chunk - run].astype(F32)], axis=0)

    def one_image(img, carry):
        first = img == 0
        last = img == own - 1

        for src in range(group):
            pltpu.make_async_copy(images.at[0], xbuf.at[img, src], recv_sem.at[img, src]).wait()

        @pl.when(img + 1 < own)
        def _():
            send_image(img + 1, 0)

        for at in range(0, rows, chunk):
            put(hbuf, layer_norm(x_rows(img, at), ln1s[...], ln1b[...]), 8, rows=slice(at, at + chunk))

        @pl.when(first)
        def _():
            arrived(0)

        for c in range(3):
            weight = blocks(wqkv, 2, rows=slice(c * width, (c + 1) * width))
            put(qkv, dot_t(blocks(hbuf, 8), weight) + bias[c:c + 1, :], 8, first=c * 8)

        lane = lax.broadcasted_iota(jnp.int32, (1, 128), 1)
        low = (lane < 64).astype(F32)
        low_b = low.astype(BF16)
        high_b = (1.0 - low).astype(BF16)
        score_mul = LOG2E * 0.125

        def one_pair(hp):
            q2, k2, v2 = qkv[hp], qkv[8 + hp], qkv[16 + hp]

            def soft(q_half):
                scores = dot_t(q_half, k2)
                top = jnp.max(scores, axis=-1, keepdims=True)
                weight = jnp.exp2((scores - top) * score_mul)
                return weight.astype(BF16), jnp.sum(weight, axis=-1, keepdims=True)

            w_lo, l_lo = soft(q2 * low_b)
            w_hi, l_hi = soft(q2 * high_b)
            total = dot(w_lo, v2 * low_b) + dot(w_hi, v2 * high_b)
            denom = jnp.where(lane < 64, l_lo, l_hi)
            ctx[hp] = (total / denom).astype(BF16)

        def head_pair(step, carry):
            one_pair(2 * step)
            one_pair(2 * step + 1)
            return carry

        lax.fori_loop(0, 4, head_pair, 0)

        @pl.when(first)
        def _():
            arrived(2)

        for at in range(0, rows, rows // 2):
            half = slice(at, at + rows // 2)
            acc[half, :] = dot(blocks(ctx, 8, rows=half), blocks(wout, 2))
        for at in range(0, rows, chunk):
            block = slice(at, at + chunk)
            r = (x_rows(img, at) + (acc[block, :] + bout[...])).astype(BF16).astype(F32)
            acc[block, :] = r + bdown[...]
            put(hbuf, layer_norm(r, ln2s[...], ln2b[...]), 8, rows=block)

        @pl.when(last)
        def _():
            start(6)

        @pl.when(first)
        def _():
            arrived(3)
            arrived(4)

        def hidden_chunk(step, carry):
            spans = [pl.ds(pl.multiple_of((2 * step + i) * width, width), width) for i in range(2)]
            for i in range(2):
                up = dot(blocks(hbuf, 8), blocks(wup, 2, first=(2 * step + i) * 2)) + bup[:, spans[i]]
                put(mbuf, gelu(up), 8, first=8 * i)
            acc[...] += dot(blocks(mbuf, 8), blocks(wdown, 2, rows=spans[0])) + dot(blocks(mbuf, 8, first=8), blocks(wdown, 2, rows=spans[1]))

            @pl.when(last)
            def _():
                for i in range(4):
                    part = step * 4 + i
                    up_cols = pl.ds(pl.multiple_of(part * 512, 512), 512)
                    pltpu.make_async_copy(pwup_hbm.at[:, up_cols], wup.at[part], w_sem.at[7]).start()
                for i in range(2):
                    down_rows = pl.ds(pl.multiple_of(step * 2 * width, width), 2 * width)
                    pltpu.make_async_copy(pwdown_hbm.at[down_rows, i * 512:(i + 1) * 512], wdown.at[i, down_rows], w_sem.at[8]).start()

            return carry

        lax.fori_loop(0, 2, hidden_chunk, 0)

        for at in range(0, rows, chunk):
            block = slice(at, at + chunk)
            y = acc[block, :].astype(BF16).astype(F32)
            put(hbuf, layer_norm(y, lnfs[...], lnfb[...]), 8, rows=block)

        @pl.when(first)
        def _():
            arrived(5)

        for c in range(2):
            weight = blocks(pwkv, 2, rows=slice(c * width, (c + 1) * width))
            put(qkv, dot_t(blocks(hbuf, 8), weight) + bias[3 + c:4 + c, :], 8, first=c * 8)
        scores = dot_t(blocks(qkv, 8), blocks(ublk, 8))
        top = jnp.max(scores, axis=0, keepdims=True)
        weight = jnp.exp2((scores - top) * score_mul)
        wsum = jnp.sum(weight, axis=0, keepdims=True)
        value = lax.dot_general(weight.astype(BF16), blocks(qkv, 8, first=8), CONTRACT_FIRST, preferred_element_type=F32)[:16]
        diag = lax.broadcasted_iota(jnp.int32, (16, 128), 0) == lax.broadcasted_iota(jnp.int32, (16, 128), 1)
        wcol = jnp.sum(jnp.where(diag, jnp.broadcast_to(wsum, (16, 128)), 0.0), axis=1, keepdims=True)
        pooled = jnp.sum(jnp.where(own_head, value / wcol, 0.0), axis=0, keepdims=True)
        abuf[pl.ds(img, 1), :] = pooled
        return carry

    lax.fori_loop(0, own, one_image, 0)

    arrived(6)
    arrived(7)
    arrived(8)
    pooled_out = (dot(abuf[...].astype(BF16), blocks(wout, 2)) + pbout[...]).astype(BF16).astype(F32)
    normed_out = layer_norm(pooled_out, plns[...], plnb[...]).astype(BF16)
    total = pooled_out + pbdown[...]
    for c in range(4):
        up = dot(normed_out, blocks(wup, 2, first=c * 2)) + pbup[:, c * 1024:(c + 1) * 1024]
        total = total + dot(gelu(up).astype(BF16), blocks(wdown, 2, rows=slice(c * 1024, (c + 1) * 1024)))
    emb[...] = total[:8]

    def drain(img, carry):
        for step in range(1, group):
            piece(img, step).wait_send()
        return carry

    lax.fori_loop(0, own, drain, 0)

    def share(step):
        return pltpu.make_async_remote_copy(
            src_ref=emb, dst_ref=gath.at[me], send_sem=gsend_sem.at[step], recv_sem=grecv_sem.at[me],
            device_id={"cp": peer(step)}, device_id_type=MESH)

    for step in range(1, group):
        share(step).start()
    gath[me] = emb[...]
    for step in range(1, group):
        src = lax.rem(me + step, group)
        pltpu.make_async_copy(emb, gath.at[src], grecv_sem.at[src]).wait()
    for step in range(1, group):
        share(step).wait_send()
    for src in range(group):
        out_ref[src * own:(src + 1) * own, :] = gath[src][:own]


def solution(mesh):
    group = mesh.shape["cp"]

    def device_step(images, ln1_scale, ln1_bias, w_qkv, b_qkv, w_out, b_out, ln2_scale, ln2_bias, w_up, b_up, w_down, b_down, lnf_scale, lnf_bias, pool_probe, pool_wq, pool_bq, pool_wkv, pool_bkv, pool_wout, pool_bout, pool_ln_scale, pool_ln_bias, pool_w_up, pool_b_up, pool_w_down, pool_b_down):
        n_img, run, width = images.shape
        own = n_img // group
        rows = group * run
        row = lambda v: v.reshape(1, -1)
        wqkv = w_qkv.transpose(1, 2, 3, 0).reshape(3 * width, width)
        pwq = pool_wq.transpose(1, 2, 0).reshape(width, width)
        pwkv = pool_wkv.transpose(1, 2, 3, 0).reshape(2 * width, width)
        any_spec = pl.BlockSpec(memory_space=pl.ANY)
        vmem_spec = pl.BlockSpec(memory_space=pltpu.VMEM)
        return pl.pallas_call(
            functools.partial(kernel, group, own, run),
            out_shape=jax.ShapeDtypeStruct((n_img, width), F32),
            in_specs=[any_spec] + [vmem_spec] * 18 + [any_spec] * 9,
            out_specs=vmem_spec,
            scratch_shapes=[
                pltpu.VMEM((own, group, run, width), BF16),
                pltpu.VMEM((2, 3 * width, 512), BF16),
                pltpu.VMEM((2, width, 512), BF16),
                pltpu.VMEM((8, width, 512), BF16),
                pltpu.VMEM((2, 4 * width, 512), BF16),
                pltpu.VMEM((2, 2 * width, 512), BF16),
                pltpu.VMEM((8, rows, 128), BF16),
                pltpu.VMEM((24, rows, 128), BF16),
                pltpu.VMEM((8, rows, 128), BF16),
                pltpu.VMEM((16, rows, 128), BF16),
                pltpu.VMEM((rows, width), F32),
                pltpu.VMEM((8, 128, 128), BF16),
                pltpu.VMEM((8, width), F32),
                pltpu.VMEM((16, width), F32),
                pltpu.VMEM((8, width), F32),
                pltpu.VMEM((group, 8, width), F32),
                pltpu.SemaphoreType.DMA((own, group)),
                pltpu.SemaphoreType.DMA((own, group)),
                pltpu.SemaphoreType.DMA((9,)),
                pltpu.SemaphoreType.DMA((group,)),
                pltpu.SemaphoreType.DMA((group,)),
            ],
            compiler_params=pltpu.CompilerParams(collective_id=0, has_side_effects=True, vmem_limit_bytes=67043328),
        )(images, row(ln1_scale), row(ln1_bias), b_qkv, row(b_out), row(ln2_scale), row(ln2_bias), row(b_up), row(b_down),
          row(lnf_scale), row(lnf_bias), pool_bq[None], pool_bkv, row(pool_bout), row(pool_ln_scale), row(pool_ln_bias),
          row(pool_b_up), row(pool_b_down), pool_probe, wqkv, w_out.reshape(width, width), w_up, w_down, pwq, pwkv,
          pool_wout.reshape(width, width), pool_w_up, pool_w_down)

    in_specs = (P("dp", "cp", None),) + (P(),) * 27
    return jax.shard_map(device_step, mesh=mesh, in_specs=in_specs, out_specs=P("dp", None), check_vma=False)
```

```python
import functools

import jax
import jax.numpy as jnp
from jax import lax
from jax.experimental import pallas as pl
from jax.experimental.pallas import tpu as pltpu
from jax.sharding import PartitionSpec as P

EPSILON = 1e-6
MESH = pl.DeviceIdType.MESH
BF16 = jnp.bfloat16
F32 = jnp.float32
LOG2E = 1.4426950408889634
CONTRACT_LAST = (((1,), (1,)), ((), ()))
CONTRACT_FIRST = (((0,), (0,)), ((), ()))

def layer_norm(values, ln_gain, ln_shift):
    row_mean = jnp.mean(values, axis=-1, keepdims=True)
    centered = values - row_mean
    variance = jnp.mean(centered * centered, axis=-1, keepdims=True)
    return centered * lax.rsqrt(variance + EPSILON) * ln_gain + ln_shift


def gelu(x):
    c0 = 0.7978845608028654
    return (0.5 * x) * (1.0 + jnp.tanh(x * (c0 + (c0 * 0.044715) * (x * x))))


def dot_t(lhs, rhs):
    return lax.dot_general(lhs, rhs, CONTRACT_LAST, preferred_element_type=F32)


def dot(lhs, rhs):
    return jnp.dot(lhs, rhs, preferred_element_type=F32)


def blocks(ref, count, first=0, rows=slice(None)):
    return jnp.concatenate([ref[first + c, rows, :] for c in range(count)], axis=1)


def put(ref, value, count, first=0, rows=slice(None)):
    for c in range(count):
        ref[first + c, rows, :] = value[:, c * 128:(c + 1) * 128].astype(BF16)


def kernel(group, own, run, images, ln1s, ln1b, bqkv_in, bout, ln2s, ln2b, bup, bdown, lnfs, lnfb, pbq_in, pbkv_in, pbout, plns, plnb, pbup, pbdown,
           probe, wqkv_hbm, wout_hbm, wup_hbm, wdown_hbm, pwq_hbm, pwkv_hbm, pwout_hbm, pwup_hbm, pwdown_hbm,
           out_ref, xbuf, wqkv, wout, wup, wdown, pwkv, h1, hbuf, qkv, ctx, mbuf, acc, ublk, bias, abuf, emb, gath,
           send_sem, recv_sem, w_sem, gsend_sem, grecv_sem):
    me = lax.axis_index("cp")
    width = 1024
    rows = group * run

    def peer(step):
        return lax.rem(me + step, group)

    weights = ((wqkv_hbm, wqkv), (pwq_hbm, pwkv.at[:, :width]), (wout_hbm, wout), (wup_hbm, wup), (wdown_hbm, wdown), (pwkv_hbm, pwkv),
               (pwout_hbm, wout), (pwup_hbm, wup), (pwdown_hbm, wdown))

    def start(k):
        src, dst = weights[k]

        def one(c, carry):
            cols = pl.ds(pl.multiple_of(c * 512, 512), 512)
            pltpu.make_async_copy(src.at[:, cols], dst.at[c], w_sem.at[k]).start()
            return carry

        lax.fori_loop(0, src.shape[1] // 512, one, 0)

    def arrived(k):
        dst = weights[k][1]
        pltpu.make_async_copy(dst, dst, w_sem.at[k]).wait()

    def piece(img, step):
        dst = peer(step)
        return pltpu.make_async_remote_copy(
            src_ref=images.at[dst * own + img], dst_ref=xbuf.at[img, me],
            send_sem=send_sem.at[img, step], recv_sem=recv_sem.at[img, me],
            device_id={"cp": dst}, device_id_type=MESH)

    def local_piece(img):
        return pltpu.make_async_copy(images.at[me * own + img], xbuf.at[img, me], recv_sem.at[img, me])

    start(0)
    start(1)
    barrier = pltpu.get_barrier_semaphore()
    for step in range(1, group):
        pl.semaphore_signal(barrier, inc=1, device_id={"cp": peer(step)}, device_id_type=MESH)
    pl.semaphore_wait(barrier, group - 1)

    def send_image(img, carry):
        local_piece(img).start()
        for step in (6, 2, 4, 7, 3, 5, 1):
            piece(img, step).start()
        return carry

    send_image(0, 0)
    for k in range(2, 5):
        start(k)

    for row, (ref, at) in enumerate(((bqkv_in, 0), (bqkv_in, 1), (bqkv_in, 2), (pbkv_in, 0), (pbkv_in, 1), (pbq_in, 0))):
        table = ref[at]
        bias[row:row + 1, :] = jnp.concatenate([table[h:h + 1, :] for h in range(16)], axis=1)

    arrived(1)
    probe_rows = jnp.broadcast_to(probe[...], (16, width))
    u = (dot_t(probe_rows, blocks(pwkv, 2, rows=slice(0, width))) + bias[5:6, :]).astype(BF16).astype(F32)
    head_of_lane = lax.broadcasted_iota(jnp.int32, (16, width), 1) // 64
    head_of_row = lax.broadcasted_iota(jnp.int32, (16, width), 0)
    own_head = head_of_lane == head_of_row
    put(ublk, jnp.concatenate([jnp.where(own_head, u, 0.0), jnp.zeros((112, width), F32)], axis=0), 8)
    start(5)
    abuf[...] = jnp.zeros_like(abuf)

    chunk = 16

    def x_rows(img, at, base=0):
        src, off = base + at // run, at % run
        if off + chunk <= run:
            return xbuf[img, src, off:off + chunk].astype(F32)
        return jnp.concatenate([xbuf[img, src, off:].astype(F32), xbuf[img, src + 1, :off + chunk - run].astype(F32)], axis=0)

    def landed(img, src):
        pltpu.make_async_copy(images.at[0], xbuf.at[img, src], recv_sem.at[img, src]).wait()

    def first_norm(img, base, count):
        for at in range(0, count * run, chunk):
            span = pl.ds(pl.multiple_of(base * run + at, chunk), chunk)
            put(h1, layer_norm(x_rows(img, at, base), ln1s[...], ln1b[...]), 8, rows=span)

    def first_image(step, carry):
        base = 2 * lax.rem(me // 2 + step, group // 2)
        landed(0, base)
        landed(0, base + 1)
        first_norm(0, base, 2)
        return carry

    lax.fori_loop(0, group // 2, first_image, 0)

    def one_image(img, carry):
        @pl.when(img + 1 < own)
        def _():
            send_image(img + 1, 0)

        first = img == 0
        last = img == own - 1

        @pl.when(first)
        def _():
            arrived(0)

        for c in range(3):
            weight = blocks(wqkv, 2, rows=slice(c * width, (c + 1) * width))
            put(qkv, dot_t(blocks(h1, 8), weight) + bias[c:c + 1, :], 8, first=c * 8)

        lane = lax.broadcasted_iota(jnp.int32, (1, 128), 1)
        low = (lane < 64).astype(F32)
        low_b = low.astype(BF16)
        high_b = (1.0 - low).astype(BF16)
        score_mul = LOG2E * 0.125

        def one_pair(hp):
            q2, k2, v2 = qkv[hp], qkv[8 + hp], qkv[16 + hp]

            def soft(q_half):
                scores = dot_t(q_half, k2)
                top = jnp.max(scores, axis=-1, keepdims=True)
                weight = jnp.exp2((scores - top) * score_mul)
                return weight.astype(BF16), jnp.sum(weight, axis=-1, keepdims=True)

            w_lo, l_lo = soft(q2 * low_b)
            w_hi, l_hi = soft(q2 * high_b)
            total = dot(w_lo, v2 * low_b) + dot(w_hi, v2 * high_b)
            denom = jnp.where(lane < 64, l_lo, l_hi)
            ctx[hp] = (total / denom).astype(BF16)

        def head_pair(step, carry):
            for i in range(4):
                one_pair(4 * step + i)
            return carry

        lax.fori_loop(0, 2, head_pair, 0)

        @pl.when(first)
        def _():
            arrived(2)

        for at in range(0, rows, rows // 2):
            half = slice(at, at + rows // 2)
            acc[half, :] = dot(blocks(ctx, 8, rows=half), blocks(wout, 2))
        for at in range(0, rows, chunk):
            block = slice(at, at + chunk)
            r = (x_rows(img, at) + (acc[block, :] + bout[...])).astype(BF16).astype(F32)
            acc[block, :] = r + bdown[...]
            put(hbuf, layer_norm(r, ln2s[...], ln2b[...]), 8, rows=block)

        @pl.when(last)
        def _():
            start(6)

        @pl.when(first)
        def _():
            arrived(3)
            arrived(4)

        @pl.when(img + 1 < own)
        def _():
            for src in range(group):
                landed(img + 1, src)

        following = jnp.minimum(img + 1, own - 1)

        def hidden_chunk(step, carry):
            first_norm(following, step * (group // 2), group // 2)
            spans = [pl.ds(pl.multiple_of((2 * step + i) * width, width), width) for i in range(2)]
            for i in range(2):
                up = dot(blocks(hbuf, 8), blocks(wup, 2, first=(2 * step + i) * 2)) + bup[:, spans[i]]
                put(mbuf, gelu(up), 8, first=8 * i)
            acc[...] += dot(blocks(mbuf, 8), blocks(wdown, 2, rows=spans[0])) + dot(blocks(mbuf, 8, first=8), blocks(wdown, 2, rows=spans[1]))

            @pl.when(last)
            def _():
                for i in range(4):
                    part = step * 4 + i
                    up_cols = pl.ds(pl.multiple_of(part * 512, 512), 512)
                    pltpu.make_async_copy(pwup_hbm.at[:, up_cols], wup.at[part], w_sem.at[7]).start()
                for i in range(2):
                    down_rows = pl.ds(pl.multiple_of(step * 2 * width, width), 2 * width)
                    pltpu.make_async_copy(pwdown_hbm.at[down_rows, i * 512:(i + 1) * 512], wdown.at[i, down_rows], w_sem.at[8]).start()

            return carry

        lax.fori_loop(0, 2, hidden_chunk, 0)

        for at in range(0, rows, chunk):
            block = slice(at, at + chunk)
            y = acc[block, :].astype(BF16).astype(F32)
            put(hbuf, layer_norm(y, lnfs[...], lnfb[...]), 8, rows=block)

        @pl.when(first)
        def _():
            arrived(5)

        for c in range(2):
            weight = blocks(pwkv, 2, rows=slice(c * width, (c + 1) * width))
            put(qkv, dot_t(blocks(hbuf, 8), weight) + bias[3 + c:4 + c, :], 8, first=c * 8)
        scores = dot_t(blocks(qkv, 8), blocks(ublk, 8))
        top = jnp.max(scores, axis=0, keepdims=True)
        weight = jnp.exp2((scores - top) * score_mul)
        wsum = jnp.sum(weight, axis=0, keepdims=True)
        value = lax.dot_general(weight.astype(BF16), blocks(qkv, 8, first=8), CONTRACT_FIRST, preferred_element_type=F32)[:16]
        diag = lax.broadcasted_iota(jnp.int32, (16, 128), 0) == lax.broadcasted_iota(jnp.int32, (16, 128), 1)
        wcol = jnp.sum(jnp.where(diag, jnp.broadcast_to(wsum, (16, 128)), 0.0), axis=1, keepdims=True)
        pooled = jnp.sum(jnp.where(own_head, value / wcol, 0.0), axis=0, keepdims=True)
        abuf[pl.ds(img, 1), :] = pooled
        return carry

    lax.fori_loop(0, own, one_image, 0)

    arrived(6)
    arrived(7)
    arrived(8)
    pooled_out = (dot(abuf[...].astype(BF16), blocks(wout, 2)) + pbout[...]).astype(BF16).astype(F32)
    normed_out = layer_norm(pooled_out, plns[...], plnb[...]).astype(BF16)
    total = pooled_out + pbdown[...]
    for c in range(4):
        up = dot(normed_out, blocks(wup, 2, first=c * 2)) + pbup[:, c * 1024:(c + 1) * 1024]
        total = total + dot(gelu(up).astype(BF16), blocks(wdown, 2, rows=slice(c * 1024, (c + 1) * 1024)))
    for c in range(8):
        emb[:, c, :] = total[:own, c * 128:(c + 1) * 128]

    def drain(img, carry):
        for step in range(1, group):
            piece(img, step).wait_send()
        return carry

    lax.fori_loop(0, own, drain, 0)

    def share(step):
        return pltpu.make_async_remote_copy(
            src_ref=emb, dst_ref=gath.at[me], send_sem=gsend_sem.at[step], recv_sem=grecv_sem.at[me],
            device_id={"cp": peer(step)}, device_id_type=MESH)

    for step in range(1, group):
        share(step).start()
    gath[me] = emb[...]
    for step in range(1, group):
        src = lax.rem(me + step, group)
        pltpu.make_async_copy(emb, gath.at[src], grecv_sem.at[src]).wait()
    for step in range(1, group):
        share(step).wait_send()
    for src in range(group):
        for c in range(8):
            out_ref[src * own:(src + 1) * own, c * 128:(c + 1) * 128] = gath[src, :, c, :]


def solution(mesh):
    group = mesh.shape["cp"]

    def device_step(images, ln1_scale, ln1_bias, w_qkv, b_qkv, w_out, b_out, ln2_scale, ln2_bias, w_up, b_up, w_down, b_down, lnf_scale, lnf_bias, pool_probe, pool_wq, pool_bq, pool_wkv, pool_bkv, pool_wout, pool_bout, pool_ln_scale, pool_ln_bias, pool_w_up, pool_b_up, pool_w_down, pool_b_down):
        n_img, run, width = images.shape
        own = n_img // group
        rows = group * run
        row = lambda v: v.reshape(1, -1)
        wqkv = w_qkv.transpose(1, 2, 3, 0).reshape(3 * width, width)
        pwq = pool_wq.transpose(1, 2, 0).reshape(width, width)
        pwkv = pool_wkv.transpose(1, 2, 3, 0).reshape(2 * width, width)
        any_spec = pl.BlockSpec(memory_space=pl.ANY)
        vmem_spec = pl.BlockSpec(memory_space=pltpu.VMEM)
        return pl.pallas_call(
            functools.partial(kernel, group, own, run),
            out_shape=jax.ShapeDtypeStruct((n_img, width), F32),
            in_specs=[any_spec] + [vmem_spec] * 18 + [any_spec] * 9,
            out_specs=vmem_spec,
            scratch_shapes=[
                pltpu.VMEM((own, group, run, width), BF16),
                pltpu.VMEM((2, 3 * width, 512), BF16),
                pltpu.VMEM((2, width, 512), BF16),
                pltpu.VMEM((8, width, 512), BF16),
                pltpu.VMEM((2, 4 * width, 512), BF16),
                pltpu.VMEM((2, 2 * width, 512), BF16),
                pltpu.VMEM((8, rows, 128), BF16),
                pltpu.VMEM((8, rows, 128), BF16),
                pltpu.VMEM((24, rows, 128), BF16),
                pltpu.VMEM((8, rows, 128), BF16),
                pltpu.VMEM((16, rows, 128), BF16),
                pltpu.VMEM((rows, width), F32),
                pltpu.VMEM((8, 128, 128), BF16),
                pltpu.VMEM((8, width), F32),
                pltpu.VMEM((16, width), F32),
                pltpu.VMEM((own, 8, 128), F32),
                pltpu.VMEM((group, own, 8, 128), F32),
                pltpu.SemaphoreType.DMA((own, group)),
                pltpu.SemaphoreType.DMA((own, group)),
                pltpu.SemaphoreType.DMA((9,)),
                pltpu.SemaphoreType.DMA((group,)),
                pltpu.SemaphoreType.DMA((group,)),
            ],
            compiler_params=pltpu.CompilerParams(collective_id=0, has_side_effects=True, vmem_limit_bytes=67043328),
        )(images, row(ln1_scale), row(ln1_bias), b_qkv, row(b_out), row(ln2_scale), row(ln2_bias), row(b_up), row(b_down),
          row(lnf_scale), row(lnf_bias), pool_bq[None], pool_bkv, row(pool_bout), row(pool_ln_scale), row(pool_ln_bias),
          row(pool_b_up), row(pool_b_down), pool_probe, wqkv, w_out.reshape(width, width), w_up, w_down, pwq, pwkv,
          pool_wout.reshape(width, width), pool_w_up, pool_w_down)

    in_specs = (P("dp", "cp", None),) + (P(),) * 27
    return jax.shard_map(device_step, mesh=mesh, in_specs=in_specs, out_specs=P("dp", None), check_vma=False)
```

```python
import functools

import jax
import jax.numpy as jnp
from jax import lax
from jax.experimental import pallas as pl
from jax.experimental.pallas import tpu as pltpu
from jax.sharding import PartitionSpec as P

EPSILON = 1e-6
MESH = pl.DeviceIdType.MESH
BF16 = jnp.bfloat16
F32 = jnp.float32
LOG2E = 1.4426950408889634
CONTRACT_LAST = (((1,), (1,)), ((), ()))
CONTRACT_FIRST = (((0,), (0,)), ((), ()))

def layer_norm(values, ln_gain, ln_shift):
    row_mean = jnp.mean(values, axis=-1, keepdims=True)
    centered = values - row_mean
    variance = jnp.mean(centered * centered, axis=-1, keepdims=True)
    return centered * lax.rsqrt(variance + EPSILON) * ln_gain + ln_shift


def gelu(x):
    c0 = 0.7978845608028654
    return (0.5 * x) * (1.0 + jnp.tanh(x * (c0 + (c0 * 0.044715) * (x * x))))


def dot_t(lhs, rhs):
    return lax.dot_general(lhs, rhs, CONTRACT_LAST, preferred_element_type=F32)


def dot(lhs, rhs):
    return jnp.dot(lhs, rhs, preferred_element_type=F32)


def blocks(ref, count, first=0, rows=slice(None)):
    return jnp.concatenate([ref[first + c, rows, :] for c in range(count)], axis=1)


def put(ref, value, count, first=0, rows=slice(None)):
    for c in range(count):
        ref[first + c, rows, :] = value[:, c * 128:(c + 1) * 128].astype(BF16)


def kernel(group, own, run, images, ln1s, ln1b, bqkv_in, bout, ln2s, ln2b, bup, bdown, lnfs, lnfb, pbq_in, pbkv_in, pbout, plns, plnb, pbup, pbdown,
           probe, wqkv_hbm, wout_hbm, wup_hbm, wdown_hbm, pwq_hbm, pwkv_hbm, pwout_hbm, pwup_hbm, pwdown_hbm,
           out_ref, xbuf, wqkv, wout, wup, wdown, pwkv, h1, hbuf, qkv, ctx, mbuf, acc, ublk, bias, abuf, emb, gath,
           send_sem, recv_sem, w_sem, gsend_sem, grecv_sem):
    me = lax.axis_index("cp")
    width = 1024
    rows = group * run

    def peer(step):
        return lax.rem(me + step, group)

    weights = ((wqkv_hbm, wqkv), (pwq_hbm, pwkv.at[:, :width]), (wout_hbm, wout), (wup_hbm, wup), (wdown_hbm, wdown), (pwkv_hbm, pwkv),
               (pwout_hbm, wout), (pwup_hbm, wup), (pwdown_hbm, wdown))

    def start(k):
        src, dst = weights[k]

        def one(c, carry):
            cols = pl.ds(pl.multiple_of(c * 512, 512), 512)
            pltpu.make_async_copy(src.at[:, cols], dst.at[c], w_sem.at[k]).start()
            return carry

        lax.fori_loop(0, src.shape[1] // 512, one, 0)

    def arrived(k):
        dst = weights[k][1]
        pltpu.make_async_copy(dst, dst, w_sem.at[k]).wait()

    def piece(img, step):
        dst = peer(step)
        return pltpu.make_async_remote_copy(
            src_ref=images.at[dst * own + img], dst_ref=xbuf.at[img, me],
            send_sem=send_sem.at[img, step], recv_sem=recv_sem.at[img, me],
            device_id={"cp": dst}, device_id_type=MESH)

    def local_piece(img):
        return pltpu.make_async_copy(images.at[me * own + img], xbuf.at[img, me], recv_sem.at[img, me])

    start(0)
    start(1)
    barrier = pltpu.get_barrier_semaphore()
    for step in range(1, group):
        pl.semaphore_signal(barrier, inc=1, device_id={"cp": peer(step)}, device_id_type=MESH)
    pl.semaphore_wait(barrier, group - 1)

    def send_image(img, carry):
        local_piece(img).start()
        for step in (6, 2, 4, 7, 3, 5, 1):
            piece(img, step).start()
        return carry

    send_image(0, 0)
    for k in range(2, 5):
        start(k)

    for row, (ref, at) in enumerate(((bqkv_in, 0), (bqkv_in, 1), (bqkv_in, 2), (pbkv_in, 0), (pbkv_in, 1), (pbq_in, 0))):
        table = ref[at]
        bias[row:row + 1, :] = jnp.concatenate([table[h:h + 1, :] for h in range(16)], axis=1)

    arrived(1)
    probe_rows = jnp.broadcast_to(probe[...], (16, width))
    u = (dot_t(probe_rows, blocks(pwkv, 2, rows=slice(0, width))) + bias[5:6, :]).astype(BF16).astype(F32)
    head_of_lane = lax.broadcasted_iota(jnp.int32, (16, width), 1) // 64
    head_of_row = lax.broadcasted_iota(jnp.int32, (16, width), 0)
    own_head = head_of_lane == head_of_row
    put(ublk, jnp.concatenate([jnp.where(own_head, u, 0.0), jnp.zeros((112, width), F32)], axis=0), 8)
    start(5)
    abuf[...] = jnp.zeros_like(abuf)

    chunk = 16

    def x_rows(img, at, base=0):
        src, off = base + at // run, at % run
        if off + chunk <= run:
            return xbuf[img, src, off:off + chunk].astype(F32)
        return jnp.concatenate([xbuf[img, src, off:].astype(F32), xbuf[img, src + 1, :off + chunk - run].astype(F32)], axis=0)

    def landed(img, src):
        pltpu.make_async_copy(images.at[0], xbuf.at[img, src], recv_sem.at[img, src]).wait()

    def first_norm(img, base, count):
        for at in range(0, count * run, chunk):
            span = pl.ds(pl.multiple_of(base * run + at, chunk), chunk)
            put(h1, layer_norm(x_rows(img, at, base), ln1s[...], ln1b[...]), 8, rows=span)

    def first_image(step, carry):
        base = 2 * lax.rem(me // 2 + step, group // 2)
        landed(0, base)
        landed(0, base + 1)
        first_norm(0, base, 2)
        return carry

    lax.fori_loop(0, group // 2, first_image, 0)

    def one_image(img, carry):
        @pl.when(img + 1 < own)
        def _():
            send_image(img + 1, 0)

        first = img == 0
        last = img == own - 1

        @pl.when(first)
        def _():
            arrived(0)

        for c in range(3):
            weight = blocks(wqkv, 2, rows=slice(c * width, (c + 1) * width))
            put(qkv, dot_t(blocks(h1, 8), weight) + bias[c:c + 1, :], 8, first=c * 8)

        lane = lax.broadcasted_iota(jnp.int32, (1, 128), 1)
        low = (lane < 64).astype(F32)
        low_b = low.astype(BF16)
        high_b = (1.0 - low).astype(BF16)
        score_mul = LOG2E * 0.125

        def one_pair(hp):
            q2, k2, v2 = qkv[hp], qkv[8 + hp], qkv[16 + hp]

            def soft(q_half):
                scores = dot_t(q_half, k2)
                top = jnp.max(scores, axis=-1, keepdims=True)
                weight = jnp.exp2((scores - top) * score_mul)
                return weight.astype(BF16), jnp.sum(weight, axis=-1, keepdims=True)

            w_lo, l_lo = soft(q2 * low_b)
            w_hi, l_hi = soft(q2 * high_b)
            total = dot(w_lo, v2 * low_b) + dot(w_hi, v2 * high_b)
            denom = jnp.where(lane < 64, l_lo, l_hi)
            ctx[hp] = (total / denom).astype(BF16)

        def head_pair(step, carry):
            for i in range(4):
                one_pair(4 * step + i)
            return carry

        lax.fori_loop(0, 2, head_pair, 0)

        @pl.when(first)
        def _():
            arrived(2)

        for at in range(0, rows, rows // 2):
            half = slice(at, at + rows // 2)
            acc[half, :] = dot(blocks(ctx, 8, rows=half), blocks(wout, 2))
        for at in range(0, rows, chunk):
            block = slice(at, at + chunk)
            r = (x_rows(img, at) + (acc[block, :] + bout[...])).astype(BF16).astype(F32)
            acc[block, :] = r + bdown[...]
            put(hbuf, layer_norm(r, ln2s[...], ln2b[...]), 8, rows=block)

        @pl.when(last)
        def _():
            start(6)

        @pl.when(first)
        def _():
            arrived(3)
            arrived(4)

        @pl.when(img + 1 < own)
        def _():
            for src in range(group):
                landed(img + 1, src)

        following = jnp.minimum(img + 1, own - 1)

        for c in range(4):
            up = dot(blocks(hbuf, 8), blocks(wup, 2, first=2 * c)) + bup[:, c * width:(c + 1) * width]
            put(mbuf, gelu(up), 8, first=8 * c)
            first_norm(following, 2 * c, 2)

        @pl.when(last)
        def _():
            start(7)

        for at in range(0, rows, rows // 2):
            half = slice(at, at + rows // 2)
            acc[half, :] = acc[half, :] + dot(blocks(mbuf, 32, rows=half), blocks(wdown, 2))
            for sub in range(at, at + rows // 2, chunk):
                block = slice(sub, sub + chunk)
                y = acc[block, :].astype(BF16).astype(F32)
                put(hbuf, layer_norm(y, lnfs[...], lnfb[...]), 8, rows=block)

        @pl.when(last)
        def _():
            start(8)

        @pl.when(first)
        def _():
            arrived(5)

        def pool_project(c):
            rhs = blocks(pwkv, 2, rows=slice(c * width, (c + 1) * width))
            put(qkv, dot_t(blocks(hbuf, 8), rhs) + bias[3 + c:4 + c, :], 8, first=c * 8)

        pool_project(0)
        scores = dot_t(blocks(qkv, 8), blocks(ublk, 8))
        top = jnp.max(scores, axis=0, keepdims=True)
        weight = jnp.exp2((scores - top) * score_mul)
        wsum = jnp.sum(weight, axis=0, keepdims=True)
        pool_project(1)
        value = lax.dot_general(weight.astype(BF16), blocks(qkv, 8, first=8), CONTRACT_FIRST, preferred_element_type=F32)[:16]
        diag = lax.broadcasted_iota(jnp.int32, (16, 128), 0) == lax.broadcasted_iota(jnp.int32, (16, 128), 1)
        wcol = jnp.sum(jnp.where(diag, jnp.broadcast_to(wsum, (16, 128)), 0.0), axis=1, keepdims=True)
        pooled = jnp.sum(jnp.where(own_head, value / wcol, 0.0), axis=0, keepdims=True)
        abuf[pl.ds(img, 1), :] = pooled
        return carry

    lax.fori_loop(0, own, one_image, 0)

    arrived(6)
    arrived(7)
    arrived(8)
    pooled_out = (dot(abuf[...].astype(BF16), blocks(wout, 2)) + pbout[...]).astype(BF16).astype(F32)
    normed_out = layer_norm(pooled_out, plns[...], plnb[...]).astype(BF16)
    total = pooled_out + pbdown[...]
    for c in range(4):
        up = dot(normed_out, blocks(wup, 2, first=c * 2)) + pbup[:, c * 1024:(c + 1) * 1024]
        total = total + dot(gelu(up).astype(BF16), blocks(wdown, 2, rows=slice(c * 1024, (c + 1) * 1024)))
    for c in range(8):
        emb[:, c, :] = total[:own, c * 128:(c + 1) * 128]

    def drain(img, carry):
        for step in range(1, group):
            piece(img, step).wait_send()
        return carry

    lax.fori_loop(0, own, drain, 0)

    def share(step):
        return pltpu.make_async_remote_copy(
            src_ref=emb, dst_ref=gath.at[me], send_sem=gsend_sem.at[step], recv_sem=grecv_sem.at[me],
            device_id={"cp": peer(step)}, device_id_type=MESH)

    for step in range(1, group):
        share(step).start()
    gath[me] = emb[...]
    for step in range(1, group):
        src = lax.rem(me + step, group)
        pltpu.make_async_copy(emb, gath.at[src], grecv_sem.at[src]).wait()
    for step in range(1, group):
        share(step).wait_send()
    for src in range(group):
        for c in range(8):
            out_ref[src * own:(src + 1) * own, c * 128:(c + 1) * 128] = gath[src, :, c, :]


def solution(mesh):
    group = mesh.shape["cp"]

    def device_step(images, ln1_scale, ln1_bias, w_qkv, b_qkv, w_out, b_out, ln2_scale, ln2_bias, w_up, b_up, w_down, b_down, lnf_scale, lnf_bias, pool_probe, pool_wq, pool_bq, pool_wkv, pool_bkv, pool_wout, pool_bout, pool_ln_scale, pool_ln_bias, pool_w_up, pool_b_up, pool_w_down, pool_b_down):
        n_img, run, width = images.shape
        own = n_img // group
        rows = group * run
        row = lambda v: v.reshape(1, -1)
        wqkv = w_qkv.transpose(1, 2, 3, 0).reshape(3 * width, width)
        pwq = pool_wq.transpose(1, 2, 0).reshape(width, width)
        pwkv = pool_wkv.transpose(1, 2, 3, 0).reshape(2 * width, width)
        any_spec = pl.BlockSpec(memory_space=pl.ANY)
        vmem_spec = pl.BlockSpec(memory_space=pltpu.VMEM)
        return pl.pallas_call(
            functools.partial(kernel, group, own, run),
            out_shape=jax.ShapeDtypeStruct((n_img, width), F32),
            in_specs=[any_spec] + [vmem_spec] * 18 + [any_spec] * 9,
            out_specs=vmem_spec,
            scratch_shapes=[
                pltpu.VMEM((own, group, run, width), BF16),
                pltpu.VMEM((2, 3 * width, 512), BF16),
                pltpu.VMEM((2, width, 512), BF16),
                pltpu.VMEM((8, width, 512), BF16),
                pltpu.VMEM((2, 4 * width, 512), BF16),
                pltpu.VMEM((2, 2 * width, 512), BF16),
                pltpu.VMEM((8, rows, 128), BF16),
                pltpu.VMEM((8, rows, 128), BF16),
                pltpu.VMEM((24, rows, 128), BF16),
                pltpu.VMEM((8, rows, 128), BF16),
                pltpu.VMEM((32, rows, 128), BF16),
                pltpu.VMEM((rows, width), F32),
                pltpu.VMEM((8, 128, 128), BF16),
                pltpu.VMEM((8, width), F32),
                pltpu.VMEM((16, width), F32),
                pltpu.VMEM((own, 8, 128), F32),
                pltpu.VMEM((group, own, 8, 128), F32),
                pltpu.SemaphoreType.DMA((own, group)),
                pltpu.SemaphoreType.DMA((own, group)),
                pltpu.SemaphoreType.DMA((9,)),
                pltpu.SemaphoreType.DMA((group,)),
                pltpu.SemaphoreType.DMA((group,)),
            ],
            compiler_params=pltpu.CompilerParams(collective_id=0, has_side_effects=True, vmem_limit_bytes=67043328),
        )(images, row(ln1_scale), row(ln1_bias), b_qkv, row(b_out), row(ln2_scale), row(ln2_bias), row(b_up), row(b_down),
          row(lnf_scale), row(lnf_bias), pool_bq[None], pool_bkv, row(pool_bout), row(pool_ln_scale), row(pool_ln_bias),
          row(pool_b_up), row(pool_b_down), pool_probe, wqkv, w_out.reshape(width, width), w_up, w_down, pwq, pwkv,
          pool_wout.reshape(width, width), pool_w_up, pool_w_down)

    in_specs = (P("dp", "cp", None),) + (P(),) * 27
    return jax.shard_map(device_step, mesh=mesh, in_specs=in_specs, out_specs=P("dp", None), check_vma=False)
```

```python
import functools

import jax
import jax.numpy as jnp
from jax import lax
from jax.experimental import pallas as pl
from jax.experimental.pallas import tpu as pltpu
from jax.sharding import PartitionSpec as P

EPSILON = 1e-6
MESH = pl.DeviceIdType.MESH
BF16 = jnp.bfloat16
F32 = jnp.float32
LOG2E = 1.4426950408889634
CONTRACT_LAST = (((1,), (1,)), ((), ()))
CONTRACT_FIRST = (((0,), (0,)), ((), ()))

def layer_norm(values, ln_gain, ln_shift):
    row_mean = jnp.mean(values, axis=-1, keepdims=True)
    centered = values - row_mean
    variance = jnp.mean(centered * centered, axis=-1, keepdims=True)
    return centered * lax.rsqrt(variance + EPSILON) * ln_gain + ln_shift


def gelu(x):
    c0 = 0.7978845608028654
    return (0.5 * x) * (1.0 + jnp.tanh(x * (c0 + (c0 * 0.044715) * (x * x))))


def dot_t(lhs, rhs):
    return lax.dot_general(lhs, rhs, CONTRACT_LAST, preferred_element_type=F32)


def dot(lhs, rhs):
    return jnp.dot(lhs, rhs, preferred_element_type=F32)


def blocks(ref, count, first=0, rows=slice(None)):
    return jnp.concatenate([ref[first + c, rows, :] for c in range(count)], axis=1)


def put(ref, value, count, first=0, rows=slice(None)):
    for c in range(count):
        ref[first + c, rows, :] = value[:, c * 128:(c + 1) * 128].astype(BF16)


def kernel(group, own, run, images, ln1s, ln1b, bqkv_in, bout, ln2s, ln2b, bup, bdown, lnfs, lnfb, pbq_in, pbkv_in, pbout, plns, plnb, pbup, pbdown,
           probe, wqkv_hbm, wout_hbm, wup_hbm, wdown_hbm, pwq_hbm, pwkv_hbm, pwout_hbm, pwup_hbm, pwdown_hbm,
           out_ref, xbuf, wqkv, wout, wup, wdown, pwkv, h1, hbuf, qkv, ctx, mbuf, acc, ublk, bias, abuf, emb, gath,
           send_sem, recv_sem, w_sem, gsend_sem, grecv_sem):
    me = lax.axis_index("cp")
    width = 1024
    rows = group * run

    def peer(step):
        return lax.rem(me + step, group)

    weights = ((wqkv_hbm, wqkv), (pwq_hbm, pwkv.at[:, :width]), (wout_hbm, wout), (wup_hbm, wup), (wdown_hbm, wdown), (pwkv_hbm, pwkv),
               (pwout_hbm, wout), (pwup_hbm, wup), (pwdown_hbm, wdown))

    def start(k):
        src, dst = weights[k]

        def one(c, carry):
            cols = pl.ds(pl.multiple_of(c * 512, 512), 512)
            pltpu.make_async_copy(src.at[:, cols], dst.at[c], w_sem.at[k]).start()
            return carry

        lax.fori_loop(0, src.shape[1] // 512, one, 0)

    def arrived(k):
        dst = weights[k][1]
        pltpu.make_async_copy(dst, dst, w_sem.at[k]).wait()

    def piece(img, step):
        dst = peer(step)
        return pltpu.make_async_remote_copy(
            src_ref=images.at[dst * own + img], dst_ref=xbuf.at[img, me],
            send_sem=send_sem.at[img, step], recv_sem=recv_sem.at[img, me],
            device_id={"cp": dst}, device_id_type=MESH)

    def local_piece(img):
        return pltpu.make_async_copy(images.at[me * own + img], xbuf.at[img, me], recv_sem.at[img, me])

    start(0)
    start(1)
    barrier = pltpu.get_barrier_semaphore()
    for step in range(1, group):
        pl.semaphore_signal(barrier, inc=1, device_id={"cp": peer(step)}, device_id_type=MESH)
    pl.semaphore_wait(barrier, group - 1)

    def send_image(img, carry):
        local_piece(img).start()
        for step in (6, 2, 4, 7, 3, 5, 1):
            piece(img, step).start()
        return carry

    send_image(0, 0)
    for k in range(2, 5):
        start(k)

    for row, (ref, at) in enumerate(((bqkv_in, 0), (bqkv_in, 1), (bqkv_in, 2), (pbkv_in, 0), (pbkv_in, 1), (pbq_in, 0))):
        table = ref[at]
        bias[row:row + 1, :] = jnp.concatenate([table[h:h + 1, :] for h in range(16)], axis=1)

    arrived(1)
    probe_rows = jnp.broadcast_to(probe[...], (16, width))
    u = (dot_t(probe_rows, blocks(pwkv, 2, rows=slice(0, width))) + bias[5:6, :]).astype(BF16).astype(F32)
    head_of_lane = lax.broadcasted_iota(jnp.int32, (16, width), 1) // 64
    head_of_row = lax.broadcasted_iota(jnp.int32, (16, width), 0)
    own_head = head_of_lane == head_of_row
    put(ublk, jnp.concatenate([jnp.where(own_head, u, 0.0), jnp.zeros((112, width), F32)], axis=0), 8)
    start(5)
    abuf[...] = jnp.zeros_like(abuf)

    chunk = 16

    def x_rows(img, at, base=0):
        src, off = base + at // run, at % run
        if off + chunk <= run:
            return xbuf[img, src, off:off + chunk].astype(F32)
        return jnp.concatenate([xbuf[img, src, off:].astype(F32), xbuf[img, src + 1, :off + chunk - run].astype(F32)], axis=0)

    def landed(img, src):
        pltpu.make_async_copy(images.at[0], xbuf.at[img, src], recv_sem.at[img, src]).wait()

    def first_norm(img, base, count):
        for at in range(0, count * run, chunk):
            span = pl.ds(pl.multiple_of(base * run + at, chunk), chunk)
            put(h1, layer_norm(x_rows(img, at, base), ln1s[...], ln1b[...]), 8, rows=span)

    def first_image(step, carry):
        base = 2 * lax.rem(me // 2 + step, group // 2)
        landed(0, base)
        landed(0, base + 1)
        if own > 1:
            @pl.when(step == group // 2 - 2)
            def _():
                send_image(1, 0)

        first_norm(0, base, 2)
        return carry

    lax.fori_loop(0, group // 2, first_image, 0)

    def one_image(img, carry):
        first = img == 0
        last = img == own - 1

        @pl.when(first)
        def _():
            arrived(0)

        for c in range(3):
            weight = blocks(wqkv, 2, rows=slice(c * width, (c + 1) * width))
            put(qkv, dot_t(blocks(h1, 8), weight) + bias[c:c + 1, :], 8, first=c * 8)

        lane = lax.broadcasted_iota(jnp.int32, (1, 128), 1)
        low = (lane < 64).astype(F32)
        low_b = low.astype(BF16)
        high_b = (1.0 - low).astype(BF16)
        score_mul = LOG2E * 0.125

        def one_pair(hp):
            q2, k2, v2 = qkv[hp], qkv[8 + hp], qkv[16 + hp]

            def soft(q_half):
                scores = dot_t(q_half, k2)
                top = jnp.max(scores, axis=-1, keepdims=True)
                weight = jnp.exp2((scores - top) * score_mul)
                return weight.astype(BF16), jnp.sum(weight, axis=-1, keepdims=True)

            w_lo, l_lo = soft(q2 * low_b)
            w_hi, l_hi = soft(q2 * high_b)
            total = dot(w_lo, v2 * low_b) + dot(w_hi, v2 * high_b)
            denom = jnp.where(lane < 64, l_lo, l_hi)
            ctx[hp] = (total / denom).astype(BF16)

        def head_pair(step, carry):
            for i in range(4):
                one_pair(4 * step + i)
            return carry

        lax.fori_loop(0, 2, head_pair, 0)

        @pl.when(first)
        def _():
            arrived(2)
            arrived(3)
            arrived(4)

        @pl.when(img + 1 < own)
        def _():
            for src in range(group):
                landed(img + 1, src)

        @pl.when(img + 2 < own)
        def _():
            send_image(img + 2, 0)

        following = jnp.minimum(img + 1, own - 1)

        for at in range(0, rows, rows // 2):
            half = slice(at, at + rows // 2)
            acc[half, :] = dot(blocks(ctx, 8, rows=half), blocks(wout, 2))
        for at in range(0, rows, chunk):
            block = slice(at, at + chunk)
            r = (x_rows(img, at) + (acc[block, :] + bout[...])).astype(BF16).astype(F32)
            acc[block, :] = r + bdown[...]
            put(hbuf, layer_norm(r, ln2s[...], ln2b[...]), 8, rows=block)

        for c in range(4):
            pieces = 2 if c == 0 else 1
            for at in range(0, rows, rows // pieces):
                part = slice(at, at + rows // pieces)
                up = dot(blocks(hbuf, 8, rows=part), blocks(wup, 2, first=2 * c)) + bup[:, c * width:(c + 1) * width]
                put(mbuf, gelu(up), 8, first=8 * c, rows=part)
            first_norm(following, 2 * c, 2)

        @pl.when(last)
        def _():
            start(6)
            start(7)

        for at in range(0, rows, rows // 2):
            half = slice(at, at + rows // 2)
            acc[half, :] = acc[half, :] + dot(blocks(mbuf, 32, rows=half), blocks(wdown, 2))
            for sub in range(at, at + rows // 2, chunk):
                block = slice(sub, sub + chunk)
                y = acc[block, :].astype(BF16).astype(F32)
                put(hbuf, layer_norm(y, lnfs[...], lnfb[...]), 8, rows=block)

        @pl.when(last)
        def _():
            start(8)

        @pl.when(first)
        def _():
            arrived(5)

        def pool_project(c):
            rhs = blocks(pwkv, 2, rows=slice(c * width, (c + 1) * width))
            put(qkv, dot_t(blocks(hbuf, 8), rhs) + bias[3 + c:4 + c, :], 8, first=c * 8)

        pool_project(0)
        scores = dot_t(blocks(qkv, 8), blocks(ublk, 8))
        top = jnp.max(scores, axis=0, keepdims=True)
        weight = jnp.exp2((scores - top) * score_mul)
        wsum = jnp.sum(weight, axis=0, keepdims=True)
        pool_project(1)
        value = lax.dot_general(weight.astype(BF16), blocks(qkv, 8, first=8), CONTRACT_FIRST, preferred_element_type=F32)[:16]
        diag = lax.broadcasted_iota(jnp.int32, (16, 128), 0) == lax.broadcasted_iota(jnp.int32, (16, 128), 1)
        wcol = jnp.sum(jnp.where(diag, jnp.broadcast_to(wsum, (16, 128)), 0.0), axis=1, keepdims=True)
        pooled = jnp.sum(jnp.where(own_head, value / wcol, 0.0), axis=0, keepdims=True)
        abuf[pl.ds(img, 1), :] = pooled
        return carry

    lax.fori_loop(0, own, one_image, 0)

    arrived(6)
    arrived(7)
    arrived(8)
    pooled_out = (dot(abuf[...].astype(BF16), blocks(wout, 2)) + pbout[...]).astype(BF16).astype(F32)
    normed_out = layer_norm(pooled_out, plns[...], plnb[...]).astype(BF16)
    total = pooled_out + pbdown[...]
    for c in range(4):
        up = dot(normed_out, blocks(wup, 2, first=c * 2)) + pbup[:, c * 1024:(c + 1) * 1024]
        total = total + dot(gelu(up).astype(BF16), blocks(wdown, 2, rows=slice(c * 1024, (c + 1) * 1024)))
    for c in range(8):
        emb[:, c, :] = total[:own, c * 128:(c + 1) * 128]

    def drain(img, carry):
        for step in range(1, group):
            piece(img, step).wait_send()
        return carry

    lax.fori_loop(0, own, drain, 0)

    def share(step):
        return pltpu.make_async_remote_copy(
            src_ref=emb, dst_ref=gath.at[me], send_sem=gsend_sem.at[step], recv_sem=grecv_sem.at[me],
            device_id={"cp": peer(step)}, device_id_type=MESH)

    for step in range(1, group):
        share(step).start()
    gath[me] = emb[...]
    for step in range(1, group):
        src = lax.rem(me + step, group)
        pltpu.make_async_copy(emb, gath.at[src], grecv_sem.at[src]).wait()
    for step in range(1, group):
        share(step).wait_send()
    for src in range(group):
        for c in range(8):
            out_ref[src * own:(src + 1) * own, c * 128:(c + 1) * 128] = gath[src, :, c, :]


def solution(mesh):
    group = mesh.shape["cp"]

    def device_step(images, ln1_scale, ln1_bias, w_qkv, b_qkv, w_out, b_out, ln2_scale, ln2_bias, w_up, b_up, w_down, b_down, lnf_scale, lnf_bias, pool_probe, pool_wq, pool_bq, pool_wkv, pool_bkv, pool_wout, pool_bout, pool_ln_scale, pool_ln_bias, pool_w_up, pool_b_up, pool_w_down, pool_b_down):
        n_img, run, width = images.shape
        own = n_img // group
        rows = group * run
        row = lambda v: v.reshape(1, -1)
        wqkv = w_qkv.transpose(1, 2, 3, 0).reshape(3 * width, width)
        pwq = pool_wq.transpose(1, 2, 0).reshape(width, width)
        pwkv = pool_wkv.transpose(1, 2, 3, 0).reshape(2 * width, width)
        any_spec = pl.BlockSpec(memory_space=pl.ANY)
        vmem_spec = pl.BlockSpec(memory_space=pltpu.VMEM)
        return pl.pallas_call(
            functools.partial(kernel, group, own, run),
            out_shape=jax.ShapeDtypeStruct((n_img, width), F32),
            in_specs=[any_spec] + [vmem_spec] * 18 + [any_spec] * 9,
            out_specs=vmem_spec,
            scratch_shapes=[
                pltpu.VMEM((own, group, run, width), BF16),
                pltpu.VMEM((2, 3 * width, 512), BF16),
                pltpu.VMEM((2, width, 512), BF16),
                pltpu.VMEM((8, width, 512), BF16),
                pltpu.VMEM((2, 4 * width, 512), BF16),
                pltpu.VMEM((2, 2 * width, 512), BF16),
                pltpu.VMEM((8, rows, 128), BF16),
                pltpu.VMEM((8, rows, 128), BF16),
                pltpu.VMEM((24, rows, 128), BF16),
                pltpu.VMEM((8, rows, 128), BF16),
                pltpu.VMEM((32, rows, 128), BF16),
                pltpu.VMEM((rows, width), F32),
                pltpu.VMEM((8, 128, 128), BF16),
                pltpu.VMEM((8, width), F32),
                pltpu.VMEM((16, width), F32),
                pltpu.VMEM((own, 8, 128), F32),
                pltpu.VMEM((group, own, 8, 128), F32),
                pltpu.SemaphoreType.DMA((own, group)),
                pltpu.SemaphoreType.DMA((own, group)),
                pltpu.SemaphoreType.DMA((9,)),
                pltpu.SemaphoreType.DMA((group,)),
                pltpu.SemaphoreType.DMA((group,)),
            ],
            compiler_params=pltpu.CompilerParams(collective_id=0, has_side_effects=True, vmem_limit_bytes=67043328),
        )(images, row(ln1_scale), row(ln1_bias), b_qkv, row(b_out), row(ln2_scale), row(ln2_bias), row(b_up), row(b_down),
          row(lnf_scale), row(lnf_bias), pool_bq[None], pool_bkv, row(pool_bout), row(pool_ln_scale), row(pool_ln_bias),
          row(pool_b_up), row(pool_b_down), pool_probe, wqkv, w_out.reshape(width, width), w_up, w_down, pwq, pwkv,
          pool_wout.reshape(width, width), pool_w_up, pool_w_down)

    in_specs = (P("dp", "cp", None),) + (P(),) * 27
    return jax.shard_map(device_step, mesh=mesh, in_specs=in_specs, out_specs=P("dp", None), check_vma=False)
```
